32 devices in a mesh: lon: 4 (over y, x), lat: 8 (over z, core).
Axes of the slice: x: 2, y: 2, z: 4, core: 2. Of those that a mesh axis runs over, the one named last changes fastest.
Arguments:
- tracers: float32 [4, 32, 64, 512], P(None, None, 'lat', 'lon'), may hold values from -6 to 6
- winds: float32 [2, 32, 64, 512], P(None, None, 'lat', 'lon'), may hold values from -0.45 to 0.45
- gases: bfloat16 [12, 32, 64, 512], P(None, None, 'lat', 'lon'), may hold values from -6 to 6
- sun_index: int32 [64, 512], P('lat', 'lon'), may hold values from 0 to 63, as said below
- block_slot: int32 [64, 4], P('lat', 'lon'), may hold values from -1 to 7, as said below
- albedo: bfloat16 [64, 512], P('lat', 'lon'), may hold values from 0.049804688 to 0.59765625
- sun_table: float32 [64], replicated, may hold values from 0.05 to 1
- solar: float32 [224], replicated, may hold values from 0.002 to 0.02
- w_first: bfloat16 [16, 64], replicated, may hold values from -1.5 to 1.5
- b_first: float32 [64], replicated, may hold values from -3 to 3
- w_second: bfloat16 [64, 64], replicated, may hold values from -0.75 to 0.75
- b_second: float32 [64], replicated, may hold values from -3 to 3
- w_third: bfloat16 [64, 224], replicated, may hold values from -0.75 to 0.75
- b_third: float32 [224], replicated, may hold values from -2 to 1
Outputs:
- tracers_out: float32 [4, 32, 64, 512], P(None, None, 'lat', 'lon')
- heating: float32 [32, 64, 512], P(None, 'lat', 'lon')
The draws below stay inside these ranges and needn't reach their ends.
Inputs may be any that keep to these rules, and one draw needn't show every extreme that they name: `block_slot`: each latitude row of one device's slab is a block of 128 columns. For the two devices at equal lat whose lon indices differ by 2, exactly 8 of their 16 blocks have a slot number of 0 or more, and these carry 0 to 7 once each; in every draw some device has all its blocks numbered. `sun_index`: 0 on every column of a block whose block_slot is -1, and 1 or more on every column of the other blocks.
All inputs are finite; a program needn't handle non-finite values.
Results may differ from the reference program's by a relative error of at most 0.0003.
Values may be sent and summed in bfloat16 or wider, within the bound.
No kernel may reach another device: no remote copies, remote signals or barrier semaphores. Data moves between devices by JAX's collectives and lax.ppermute only.
A program may use at most 64 MiB of HBM per device.

```python
import math
import jax
import jax.numpy as jnp
from jax import lax

LEV = 32
CLAT = 8
CLON = 128
NTR = 4
FEAT = 16
HID = 64
BANDS = 224
NSUN = 64
PRE_STEPS = 2
POST_STEPS = 2
GAS = 12
NLAT = 64
NLON = 512
N_LON = 4


def lit_layout(key):
    lat_devices = NLAT // CLAT
    lon_devices = NLON // CLON
    pairs = lon_devices // 2
    groups = lat_devices * pairs
    base = jax.random.fold_in(key, 11)
    key_mode, key_order, key_slot = jax.random.split(base, 3)
    modes = jax.random.randint(key_mode, (groups,), 0, 3)
    modes = modes.at[0].set(0)
    order = jax.vmap(lambda subkey: jax.random.permutation(subkey, 2 * CLAT))(jax.random.split(key_order, groups))
    ranks = jnp.argsort(order, axis=1, stable=True)
    sides = jnp.arange(2 * CLAT) // CLAT
    mixed = ranks < CLAT
    lit = jnp.where(modes[:, None] == 0, sides[None, :] == 0, jnp.where(modes[:, None] == 1, sides[None, :] == 1, mixed))
    position = jnp.cumsum(lit.astype(jnp.int32), axis=1) - 1
    slot_order = jax.vmap(lambda subkey: jax.random.permutation(subkey, CLAT))(jax.random.split(key_slot, groups))
    picked = jnp.take_along_axis(slot_order, jnp.clip(position, 0, CLAT - 1), 1)
    slots = jnp.where(lit, picked, -1).astype(jnp.int32)
    slots = slots.reshape(lat_devices, pairs, 2, CLAT).transpose(0, 3, 2, 1).reshape(NLAT, lon_devices)
    return slots


def draw_block_slot(key, part):
    return lit_layout(key)


def draw_sun_index(key, part):
    slots = lit_layout(key)
    lit = jnp.repeat(slots >= 0, CLON, axis=1)
    entries = jax.random.randint(jax.random.fold_in(key, 23), (NLAT, NLON), 1, NSUN)
    return jnp.where(lit, entries, 0).astype(jnp.int32)


def block_scale(rng, extent, cuts, least, largest):
    factor_of = 1.0
    for dim, blocks in cuts:
        heights = jax.random.uniform(jax.random.fold_in(jax.random.fold_in(rng, 6), dim), (blocks,), jnp.float32, least / len(cuts), largest / len(cuts))
        factor_of = factor_of * jnp.repeat(jnp.exp(heights), extent[dim] // blocks).reshape((-1,) + (1,) * (len(extent) - 1 - dim))
    return factor_of


def centred(own_key, shape, deviation, reach, cuts=(), dtype=jnp.bfloat16):
    gain = block_scale(own_key, shape, cuts, -0.22, 0.18) if cuts else 1.0
    values = jax.random.normal(own_key, shape, jnp.float32) * deviation * gain
    return jnp.minimum(jnp.maximum(values, -reach), reach).astype(dtype)


def setup_inputs(seed: int = 0) -> dict:
    key_of = jax.random.split(jax.random.key(seed), 15)
    return {
        "tracers": centred(key_of[0], (NTR, LEV, NLAT, NLON), 1.0, 6.0, ((2, 8), (3, 4)), jnp.float32),
        "winds": jnp.clip(jax.random.uniform(key_of[1], (2, LEV, NLAT, NLON), jnp.float32, -0.45, 0.45) * block_scale(key_of[1], (2, LEV, NLAT, NLON), ((2, 8), (3, 4)), -0.4, 0.0), -0.45, 0.45),
        "gases": centred(key_of[2], (GAS, LEV, NLAT, NLON), 1.0, 6.0, ((2, 8), (3, 4))),
        "sun_index": draw_sun_index(jax.random.fold_in(key_of[14], 71), 0),
        "block_slot": draw_block_slot(jax.random.fold_in(key_of[14], 71), 0),
        "albedo": jnp.clip(0.049804688 + 0.54785156 * jax.random.uniform(key_of[5], (NLAT, NLON), jnp.float32) ** block_scale(key_of[5], (NLAT, NLON), ((0, 8), (1, 4)), -0.2, 0.2), 0.049804688, 0.59765625).astype(jnp.bfloat16),
        "sun_table": jnp.clip(jax.random.uniform(key_of[6], (NSUN,), jnp.float32, 0.05, 1.0), 0.05, 1.0),
        "solar": jnp.clip(jnp.exp(jax.random.uniform(key_of[7], (BANDS,), jnp.float32, math.log(0.002), math.log(0.02))), 0.002, 0.02),
        "w_first": centred(key_of[8], (FEAT, HID), FEAT ** -0.5, 1.5),
        "b_first": centred(key_of[9], (HID,), 0.5, 3.0, (), jnp.float32),
        "w_second": centred(key_of[10], (HID, HID), HID ** -0.5, 0.75),
        "b_second": centred(key_of[11], (HID,), 0.5, 3.0, (), jnp.float32),
        "w_third": centred(key_of[12], (HID, BANDS), HID ** -0.5, 0.75),
        "b_third": jnp.clip(jax.random.uniform(key_of[13], (BANDS,), jnp.float32, -2.0, 1.0), -2.0, 1.0),
    }


tau_scale = 0.05
mu_floor = 0.05
heat_scale = 30.0
diffuse_factor = 1.66


def advance(padded, courant):
    along = courant[0]
    across = courant[1]
    rows_mid = padded[:, :, 1:-1, :]
    along_mid = along[:, 1:-1, :]
    face_east = 0.5 * (along_mid[..., :-1] + along_mid[..., 1:])
    east_flux = jnp.maximum(face_east, 0.0) * rows_mid[..., :-1] + jnp.minimum(face_east, 0.0) * rows_mid[..., 1:]
    cols_mid = padded[:, :, :, 1:-1]
    across_mid = across[:, :, 1:-1]
    face_north = 0.5 * (across_mid[:, :-1, :] + across_mid[:, 1:, :])
    north_flux = jnp.maximum(face_north, 0.0) * cols_mid[:, :, :-1, :] + jnp.minimum(face_north, 0.0) * cols_mid[:, :, 1:, :]
    return padded[:, :, 1:-1, 1:-1] - (east_flux[..., 1:] - east_flux[..., :-1]) - (north_flux[:, :, 1:, :] - north_flux[:, :, :-1, :])


def pad_global(field):
    padded = jnp.pad(field, ((0, 0), (0, 0), (1, 1), (0, 0)))
    return jnp.concatenate([padded[..., -1:], padded, padded[..., :1]], -1)


def radiate(feat_rows, index_row, ground, sun_table, solar, weights):
    w_first, b_first, w_second, b_second, w_third, b_third = weights
    featn = w_first.shape[0]
    levels = feat_rows.shape[0] // featn
    width = feat_rows.shape[1]
    inputs = feat_rows.reshape(featn, levels * width)
    hidden = jnp.dot(w_first.T, inputs, preferred_element_type=jnp.float32) + b_first[:, None]
    hidden = jax.nn.silu(hidden).astype(jnp.bfloat16)
    hidden = jnp.dot(w_second.T, hidden, preferred_element_type=jnp.float32) + b_second[:, None]
    hidden = jax.nn.silu(hidden).astype(jnp.bfloat16)
    logits = jnp.dot(w_third.T, hidden, preferred_element_type=jnp.float32) + b_third[:, None]
    optical = (tau_scale * jax.nn.softplus(logits)).reshape(-1, levels, width)
    entries = jnp.arange(sun_table.shape[0]).astype(jnp.float32)
    hits = (index_row[None, :] == entries[:, None]) & (entries[:, None] > 0.0)
    cosine = jnp.sum(jnp.where(hits, sun_table[:, None], 0.0), 0)
    safe = jnp.maximum(cosine, mu_floor)
    depth = jnp.cumsum(optical, axis=1)
    above = depth - optical
    total = depth[:, -1:, :]
    below = total - depth
    top_flux = solar[:, None, None] * cosine[None, None, :]
    direct = top_flux * jnp.exp(-above / safe) * (1.0 - jnp.exp(-optical / safe))
    upward = ground[None, None, :] * top_flux * jnp.exp(-total / safe) * jnp.exp(-diffuse_factor * below) * (1.0 - jnp.exp(-diffuse_factor * optical))
    return heat_scale * jnp.sum(direct + upward, 0)


def reference(tracers, winds, gases, sun_index, block_slot, albedo, sun_table, solar, w_first, b_first, w_second, b_second, w_third, b_third):
    weights = (w_first, b_first, w_second, b_second, w_third, b_third)
    wind_pad = pad_global(winds)
    state = tracers
    for section in range(PRE_STEPS):
        state = advance(pad_global(state), wind_pad)
    features = jnp.concatenate([gases, state.astype(jnp.bfloat16)], 0)
    blocks = features.reshape(FEAT, LEV, NLAT, N_LON, CLON).transpose(2, 3, 0, 1, 4).reshape(NLAT * N_LON, FEAT * LEV, CLON)
    indices = sun_index.reshape(NLAT * N_LON, CLON).astype(jnp.float32)
    grounds = albedo.reshape(NLAT * N_LON, CLON).astype(jnp.float32)
    lit_blocks = block_slot.reshape(NLAT * N_LON) >= 0

    def one_block(items):
        feat_rows, index_row, ground, lit = items
        return lax.cond(lit, lambda operands: radiate(operands[0], operands[1], operands[2], sun_table, solar, weights),
                        lambda operands: jnp.zeros((LEV, CLON), jnp.float32), (feat_rows, index_row, ground))

    heat_blocks = lax.map(one_block, (blocks, indices, grounds, lit_blocks))
    heating = heat_blocks.reshape(NLAT, N_LON, LEV, CLON).transpose(2, 0, 1, 3).reshape(LEV, NLAT, NLON)
    state = state.at[0].add(heating)
    for section in range(POST_STEPS):
        state = advance(pad_global(state), wind_pad)
    return state, heating
```

```python
import functools
import math

import jax
import jax.numpy as jnp
from jax import lax
from jax.experimental import pallas as pl
from jax.experimental.pallas import tpu as pltpu
from jax.sharding import PartitionSpec as P

tau_scale = 0.05
mu_floor = 0.05
heat_scale = 30.0
diffuse_factor = 1.66
log2e = 1.4426950408889634

ROWS = 8
COLS = 128
RIM = 2
SLOTS = COLS // RIM


def lane_id():
    return lax.broadcasted_iota(jnp.int32, (ROWS, COLS), 1)


def row_id():
    return lax.broadcasted_iota(jnp.int32, (ROWS, COLS), 0)


def ahead_col(tile, beside):
    return pltpu.roll(jnp.where(lane_id() == 0, beside, tile), COLS - 1, 1)


def behind_col(tile, beside):
    return pltpu.roll(jnp.where(lane_id() == COLS - 1, beside, tile), 1, 1)


def ahead_row(tile, beside):
    return pltpu.roll(jnp.where(row_id() == 0, beside, tile), ROWS - 1, 0)


def behind_row(tile, beside):
    return pltpu.roll(jnp.where(row_id() == ROWS - 1, beside, tile), 1, 0)


def flux(face, here, there):
    return jnp.maximum(face, 0.0) * here + jnp.minimum(face, 0.0) * there


def faces(along, across):
    am, ah, av, ac = along
    bm, bh, bv, bc = across
    east = tuple(
        0.5 * (t + ahead_col(t, o)) for t, o in ((am, ah), (ah, am), (av, ac), (ac, av))
    )
    north = tuple(
        0.5 * (t + ahead_row(t, o)) for t, o in ((bm, bv), (bh, bc), (bv, bm), (bc, bh))
    )
    return east, north


def two_steps(q, east, north, inside):
    m, h, v, c = q
    em = flux(east[0], m, ahead_col(m, h))
    eh = flux(east[1], h, ahead_col(h, m))
    ev = flux(east[2], v, ahead_col(v, c))
    ec = flux(east[3], c, ahead_col(c, v))
    nm = flux(north[0], m, ahead_row(m, v))
    nh = flux(north[1], h, ahead_row(h, c))
    nv = flux(north[2], v, ahead_row(v, m))
    nc = flux(north[3], c, ahead_row(c, h))
    m1 = m - (em - behind_col(em, eh)) - (nm - behind_row(nm, nv))
    h1 = h - (eh - behind_col(eh, em)) - (nh - behind_row(nh, nc))
    v1 = v - (ev - behind_col(ev, ec)) - (nv - behind_row(nv, nm))
    v1 = jnp.where(inside > 0.0, v1, 0.0)
    em = flux(east[0], m1, ahead_col(m1, h1))
    eh = flux(east[1], h1, ahead_col(h1, m1))
    nm = flux(north[0], m1, ahead_row(m1, v1))
    nv = flux(north[2], v1, ahead_row(v1, m1))
    return m1 - (em - behind_col(em, eh)) - (nm - behind_row(nm, nv))


def pack_sides(tile, slot, packs):
    head, tail = packs
    lane = lane_id()
    here = (lane >= RIM * slot) & (lane < RIM * slot + RIM)
    head = jnp.where(here, pltpu.roll(tile, RIM * slot, 1), head)
    tail = jnp.where(here, pltpu.roll(tile, lax.rem(RIM * slot + RIM, COLS), 1), tail)
    return head, tail


def unpack_sides(from_right, from_left, slot):
    right = pltpu.roll(from_right, lax.rem(COLS - RIM * slot, COLS), 1)
    left = pltpu.roll(from_left, lax.rem(2 * COLS - RIM - RIM * slot, COLS), 1)
    return jnp.where(lane_id() < COLS // 2, right, left)


def place(field, level, levels):
    per = SLOTS // levels
    return field // per, (field % per) * levels + level


def packed_tiles(fields, levels):
    return pl.cdiv(fields * levels, SLOTS)


def pack_fields(sources, levels, head_ref, tail_ref):
    count = packed_tiles(len(sources), levels)
    zero = jnp.zeros((ROWS, COLS), jnp.float32)

    def step(level, packs):
        packs = list(packs)
        for field, source in enumerate(sources):
            tile, slot = place(field, level, levels)
            packs[tile] = pack_sides(source(level), slot, packs[tile])
        return tuple(packs)

    packs = lax.fori_loop(0, levels, step, ((zero, zero),) * count)
    for tile, (head, tail) in enumerate(packs):
        head_ref[tile] = head
        tail_ref[tile] = tail


def pack_cols_kernel(tracers, winds, head, tail):
    levels = tracers.shape[1]
    fields = [(tracers, f) for f in range(tracers.shape[0])]
    fields += [(winds, f) for f in range(winds.shape[0])]
    pack_fields(
        [lambda level, ref=ref, f=f: ref[f, level] for ref, f in fields], levels, head, tail
    )


def row_payload(fields, levels):
    rows = RIM * fields * levels + 2 * RIM * packed_tiles(fields, levels)
    return -(-rows // 16) * 16


def pack_rows_kernel(*refs):
    *fields, from_right, from_left, head, tail = refs
    at = 0
    total = sum(ref.shape[0] for ref in fields) // ROWS
    for ref in fields:
        tiles = ref.shape[0] // ROWS
        for row in range(RIM):
            head[pl.ds(row * total + at, tiles), :] = ref[pl.ds(row, tiles, stride=ROWS), :]
            tail[pl.ds(row * total + at, tiles), :] = ref[
                pl.ds(ROWS - RIM + row, tiles, stride=ROWS), :
            ]
        at += tiles
    base = RIM * total
    head[base:, :] = jnp.zeros((head.shape[0] - base, COLS), jnp.float32)
    tail[base:, :] = jnp.zeros((head.shape[0] - base, COLS), jnp.float32)
    at = base
    for ref in (from_right, from_left):
        for tile in range(ref.shape[0]):
            head[at : at + RIM, :] = ref[tile, 0:RIM, :]
            tail[at : at + RIM, :] = ref[tile, ROWS - RIM : ROWS, :]
            at += RIM


def unpack_rows(from_north, from_south, rim_ref, corner_ref, tiles, packed):
    for row in range(RIM):
        rim_ref[pl.ds(row, tiles, stride=ROWS), :] = from_north[pl.ds(row * tiles, tiles), :]
        rim_ref[pl.ds(ROWS - RIM + row, tiles, stride=ROWS), :] = from_south[
            pl.ds(row * tiles, tiles), :
        ]
    at = RIM * tiles
    for tile in range(2 * packed):
        corner_ref[tile, 0:RIM, :] = from_north[at : at + RIM, :]
        corner_ref[tile, ROWS - RIM : ROWS, :] = from_south[at : at + RIM, :]
        at += RIM


def rim_tiles(field, level, levels, packed, right, left, rim_ref, corner_ref):
    tile, slot = place(field, level, levels)
    side = unpack_sides(right[tile], left[tile], slot)
    row = pl.multiple_of((field * levels + level) * ROWS, ROWS)
    rows = rim_ref[pl.ds(row, ROWS), :]
    corner = unpack_sides(corner_ref[tile], corner_ref[packed + tile], slot)
    return side, rows, corner


def first_kernel(
    tracers,
    winds,
    right,
    left,
    north,
    south,
    inside,
    gases,
    index,
    ground,
    table,
    lsolar,
    w1,
    b1,
    w2,
    b2,
    w3,
    state,
    heating,
    head,
    tail,
    rim_ref,
    corner_ref,
    xs,
    depth,
    weight,
    sums,
    kappa,
    lground,
):
    ntr, levels = tracers.shape[0], tracers.shape[1]
    fields = ntr + winds.shape[0]
    packed = packed_tiles(fields, levels)
    groups = lsolar.shape[0]
    hid = b1.shape[0]
    unpack_rows(north, south, rim_ref, corner_ref, fields * levels, packed)
    keep = inside[...]

    def transport(level, carry):
        rim = functools.partial(
            rim_tiles,
            level=level,
            levels=levels,
            packed=packed,
            right=right,
            left=left,
            rim_ref=rim_ref,
            corner_ref=corner_ref,
        )
        east, north_face = faces(
            (winds[0, level], *rim(ntr)), (winds[1, level], *rim(ntr + 1))
        )
        out = []
        for f in range(ntr):
            q = two_steps((tracers[f, level], *rim(f)), east, north_face, keep)
            state[f, level] = q
            out.append(q)
        xs[level] = jnp.concatenate(out, 0).astype(jnp.bfloat16)
        return carry

    lax.fori_loop(0, levels, transport, 0)

    ids = index[...]
    cosine = jnp.zeros((ROWS, COLS), jnp.float32)
    for entry in range(1, table.shape[0]):
        cosine = jnp.where(ids == entry, table[entry], cosine)
    slant = tau_scale / jnp.maximum(cosine, mu_floor)
    lg = jnp.log2(ground[...])
    for row in range(ROWS):
        kappa[row] = jnp.broadcast_to(slant[row : row + 1], (ROWS, COLS))
        lground[row] = jnp.broadcast_to(lg[row : row + 1], (ROWS, COLS))

    diffuse = diffuse_factor * tau_scale
    zero = jnp.zeros((groups, ROWS, COLS), jnp.float32)
    depth[0, 0] = zero
    depth[1, 0] = zero
    ones = jnp.ones((w3.shape[1] - hid, 2 * COLS), jnp.bfloat16)

    def optical(row, pair):
        buf = lax.rem(row, 2)
        l0 = 2 * pair
        x = jnp.concatenate(
            [jnp.concatenate([gases[l0 + k], xs[l0 + k]], 0) for k in range(2)], 1
        )
        wide1 = jnp.concatenate([b1[...]] * 2, 1)
        wide2 = jnp.concatenate([b2[...]] * 2, 1)
        mine = w1[pl.ds(pl.multiple_of(row * hid, hid), hid), :]
        y = jnp.dot(mine, x, preferred_element_type=jnp.float32) + wide1
        y = (y + y * jnp.tanh(y)).astype(jnp.bfloat16)
        y = jnp.dot(w2[...], y, preferred_element_type=jnp.float32) + wide2
        y = (y + y * jnp.tanh(y)).astype(jnp.bfloat16)
        y = jnp.concatenate([y, ones], 0)
        t = jnp.dot(w3[...], y, preferred_element_type=jnp.float32) * log2e
        soft = jnp.maximum(t, jnp.log2(1.0 + jnp.exp2(jnp.minimum(t, 126.0))))
        soft = soft.reshape(groups, ROWS, 2 * COLS)
        d = depth[buf, l0] + soft[:, :, :COLS]
        depth[buf, l0 + 1] = d
        depth[buf, l0 + 2] = d + soft[:, :, COLS:]

    def light(row, level):
        buf = lax.rem(row, 2)
        d = depth[buf, level]
        direct = jnp.exp2(lsolar[...] - d * kappa[row][None])
        upward = jnp.exp2(weight[...] + d * diffuse)
        sums[row, level] = jnp.sum(direct - upward, 0)

    def close(row):
        buf = lax.rem(row, 2)
        total = depth[buf, levels]
        weight[...] = (
            lsolar[...] + lground[row][None] - total * (kappa[row] + diffuse)[None]
        )
        light(row, levels)

    def lights(row, pair):
        light(row, 2 * pair)
        light(row, 2 * pair + 1)

    pairs = levels // 2

    def only_optical(pair, carry):
        optical(0, pair)
        return carry

    lax.fori_loop(0, pairs, only_optical, 0)

    def one_row(row, carry):
        close(row - 1)

        def both(pair, inner):
            optical(row, pair)
            lights(row - 1, pair)
            return inner

        return lax.fori_loop(0, pairs, both, carry)

    lax.fori_loop(1, ROWS, one_row, 0)
    close(ROWS - 1)

    def only_light(pair, carry):
        lights(ROWS - 1, pair)
        return carry

    lax.fori_loop(0, pairs, only_light, 0)

    scaled = heat_scale * cosine
    for row in range(ROWS):
        change = sums[row, 0:levels] - sums[row, 1 : levels + 1]
        heating[:, row, :] = jnp.sum(change, 1) * scaled[row : row + 1]

    def add(level, carry):
        state[0, level] = state[0, level] + heating[level]
        return carry

    lax.fori_loop(0, levels, add, 0)
    pack_fields(
        [lambda level, f=f: state[f, level] for f in range(ntr)], levels, head, tail
    )


def last_kernel(
    tracers,
    winds,
    right,
    left,
    north,
    south,
    wind_right,
    wind_left,
    wind_north,
    wind_south,
    inside,
    out,
    rim_ref,
    corner_ref,
    wind_rim_ref,
    wind_corner_ref,
):
    ntr, levels = tracers.shape[0], tracers.shape[1]
    fields = ntr + winds.shape[0]
    packed = packed_tiles(ntr, levels)
    wind_packed = packed_tiles(fields, levels)
    unpack_rows(north, south, rim_ref, corner_ref, ntr * levels, packed)
    unpack_rows(
        wind_north, wind_south, wind_rim_ref, wind_corner_ref, fields * levels, wind_packed
    )
    keep = inside[...]

    def transport(level, carry):
        rim = functools.partial(
            rim_tiles,
            level=level,
            levels=levels,
            packed=packed,
            right=right,
            left=left,
            rim_ref=rim_ref,
            corner_ref=corner_ref,
        )
        wind_rim = functools.partial(
            rim_tiles,
            level=level,
            levels=levels,
            packed=wind_packed,
            right=wind_right,
            left=wind_left,
            rim_ref=wind_rim_ref,
            corner_ref=wind_corner_ref,
        )
        east, north_face = faces(
            (winds[0, level], *wind_rim(ntr)), (winds[1, level], *wind_rim(ntr + 1))
        )
        for f in range(ntr):
            out[f, level] = two_steps((tracers[f, level], *rim(f)), east, north_face, keep)
        return carry

    lax.fori_loop(0, levels, transport, 0)


vmem = pl.BlockSpec(memory_space=pltpu.VMEM)
smem = pl.BlockSpec(memory_space=pltpu.SMEM)
f32 = jnp.float32


def tiles_like(*shape):
    return jax.ShapeDtypeStruct(shape, f32)


def shift(x, axis, by, wrap):
    count = lax.axis_size(axis)
    return lax.ppermute(
        x, axis, [(i, (i + by) % count) for i in range(count) if wrap or 0 <= i + by < count]
    )


def exchange_cols(head, tail):
    return shift(head, "lon", -1, True), shift(tail, "lon", 1, True)


def exchange_rows(fields, right, left, levels):
    count = sum(f.shape[0] for f in fields)
    rows = row_payload(count, levels)
    head, tail = pl.pallas_call(
        pack_rows_kernel,
        in_specs=[vmem] * (len(fields) + 2),
        out_specs=[vmem] * 2,
        out_shape=[tiles_like(rows, COLS)] * 2,
        name="pack_rows",
    )(*[f.reshape(-1, COLS) for f in fields], right, left)
    return shift(head, "lat", -1, False), shift(tail, "lat", 1, False)


def split3(x):
    hi = lax.reduce_precision(x, 8, 7)
    mid = lax.reduce_precision(x - hi, 8, 7)
    return [hi, mid, x - hi - mid]


def body(
    tracers,
    winds,
    gases,
    sun_index,
    block_slot,
    albedo,
    sun_table,
    solar,
    w_first,
    b_first,
    w_second,
    b_second,
    w_third,
    b_third,
):
    ntr, levels, clat, width = tracers.shape
    fields = ntr + winds.shape[0]
    gas = gases.shape[0]
    hid = w_first.shape[1]
    bands = solar.shape[0]
    if (clat, width) != (ROWS, COLS) or levels % 2 or SLOTS % levels or bands % ROWS:
        raise ValueError("unsupported sizes")

    head, tail = pl.pallas_call(
        pack_cols_kernel,
        in_specs=[vmem] * 2,
        out_specs=[vmem] * 2,
        out_shape=[tiles_like(packed_tiles(fields, levels), ROWS, COLS)] * 2,
        name="pack_cols",
    )(tracers, winds)
    right, left = exchange_cols(head, tail)
    north, south = exchange_rows((tracers, winds), right, left, levels)

    lat = lax.axis_index("lat")
    row = jnp.arange(ROWS)[:, None]
    inside = jnp.where(row == 0, lat < lax.axis_size("lat") - 1, (row == ROWS - 1) & (lat > 0))
    inside = jnp.broadcast_to(inside.astype(f32), (ROWS, COLS))
    gas_rows = gases.transpose(1, 0, 2, 3).reshape(levels, gas * ROWS, COLS)
    index = jnp.where(block_slot >= 0, sun_index, 0)
    ground = albedo.astype(f32)
    lsolar = jnp.broadcast_to(jnp.log2(solar)[:, None], (bands, COLS))
    lsolar = lsolar.reshape(bands // ROWS, ROWS, COLS)
    eye = jnp.eye(ROWS, dtype=jnp.bfloat16)
    w1 = (0.5 * w_first.T)[None, :, :, None] * eye[:, None, None, :]
    w1 = w1.reshape(ROWS * hid, -1).astype(jnp.bfloat16)
    b1 = jnp.broadcast_to(0.5 * b_first[:, None], (hid, COLS))
    w2 = (0.5 * w_second.T).astype(jnp.bfloat16)
    b2 = jnp.broadcast_to(0.5 * b_second[:, None], (hid, COLS))
    extra = [b[:, None].astype(jnp.bfloat16) for b in split3(b_third)]
    w3 = jnp.concatenate(
        [w_third.T, *extra, jnp.zeros((bands, 16 - len(extra)), jnp.bfloat16)], 1
    )

    packed = packed_tiles(fields, levels)
    state, heating, head, tail = pl.pallas_call(
        first_kernel,
        in_specs=[vmem] * 10 + [smem] + [vmem] * 6,
        out_specs=[vmem] * 4,
        out_shape=[
            tiles_like(ntr, levels, ROWS, COLS),
            tiles_like(levels, ROWS, COLS),
        ]
        + [tiles_like(packed_tiles(ntr, levels), ROWS, COLS)] * 2,
        scratch_shapes=[
            pltpu.VMEM((fields * levels * ROWS, COLS), f32),
            pltpu.VMEM((2 * packed, ROWS, COLS), f32),
            pltpu.VMEM((levels, ntr * ROWS, COLS), jnp.bfloat16),
            pltpu.VMEM((2, levels + 1, bands // ROWS, ROWS, COLS), f32),
            pltpu.VMEM((bands // ROWS, ROWS, COLS), f32),
            pltpu.VMEM((ROWS, levels + 1, ROWS, COLS), f32),
            pltpu.VMEM((ROWS, ROWS, COLS), f32),
            pltpu.VMEM((ROWS, ROWS, COLS), f32),
        ],
        name="transport_radiation",
    )(
        tracers,
        winds,
        right,
        left,
        north,
        south,
        inside,
        gas_rows,
        index,
        ground,
        sun_table,
        lsolar,
        w1,
        b1,
        w2,
        b2,
        w3,
    )

    right2, left2 = exchange_cols(head, tail)
    north2, south2 = exchange_rows((state,), right2, left2, levels)
    packed2 = packed_tiles(ntr, levels)
    final = pl.pallas_call(
        last_kernel,
        in_specs=[vmem] * 11,
        out_specs=vmem,
        out_shape=tiles_like(ntr, levels, ROWS, COLS),
        scratch_shapes=[
            pltpu.VMEM((ntr * levels * ROWS, COLS), f32),
            pltpu.VMEM((2 * packed2, ROWS, COLS), f32),
            pltpu.VMEM((fields * levels * ROWS, COLS), f32),
            pltpu.VMEM((2 * packed, ROWS, COLS), f32),
        ],
        name="last_transport",
    )(state, winds, right2, left2, north2, south2, right, left, north, south, inside)
    return final, heating


def solution(mesh):
    grid = P(None, None, "lat", "lon")
    in_specs = (grid, grid, grid) + (P("lat", "lon"),) * 3 + (P(),) * 8
    out_specs = (grid, P(None, "lat", "lon"))
    return jax.shard_map(body, mesh=mesh, in_specs=in_specs, out_specs=out_specs, check_vma=False)
```

```python
import functools
import math

import jax
import jax.numpy as jnp
from jax import lax
from jax.experimental import pallas as pl
from jax.experimental.pallas import tpu as pltpu
from jax.sharding import PartitionSpec as P

tau_scale = 0.05
mu_floor = 0.05
heat_scale = 30.0
diffuse_factor = 1.66
log2e = 1.4426950408889634

ROWS = 8
COLS = 128
RIM = 2
SLOTS = COLS // RIM


def lane_id():
    return lax.broadcasted_iota(jnp.int32, (ROWS, COLS), 1)


def row_id():
    return lax.broadcasted_iota(jnp.int32, (ROWS, COLS), 0)


def ahead_col(tile, beside):
    return pltpu.roll(jnp.where(lane_id() == 0, beside, tile), COLS - 1, 1)


def behind_col(tile, beside):
    return pltpu.roll(jnp.where(lane_id() == COLS - 1, beside, tile), 1, 1)


def ahead_row(tile, beside):
    return pltpu.roll(jnp.where(row_id() == 0, beside, tile), ROWS - 1, 0)


def behind_row(tile, beside):
    return pltpu.roll(jnp.where(row_id() == ROWS - 1, beside, tile), 1, 0)


def flux(face, here, there):
    return jnp.maximum(face, 0.0) * here + jnp.minimum(face, 0.0) * there


def faces(along, across):
    am, ah, av, ac = along
    bm, bh, bv, bc = across
    east = tuple(
        0.5 * (t + ahead_col(t, o)) for t, o in ((am, ah), (ah, am), (av, ac), (ac, av))
    )
    north = tuple(
        0.5 * (t + ahead_row(t, o)) for t, o in ((bm, bv), (bh, bc), (bv, bm), (bc, bh))
    )
    return east, north


def two_steps(q, east, north, inside):
    m, h, v, c = q
    em = flux(east[0], m, ahead_col(m, h))
    eh = flux(east[1], h, ahead_col(h, m))
    ev = flux(east[2], v, ahead_col(v, c))
    ec = flux(east[3], c, ahead_col(c, v))
    nm = flux(north[0], m, ahead_row(m, v))
    nh = flux(north[1], h, ahead_row(h, c))
    nv = flux(north[2], v, ahead_row(v, m))
    nc = flux(north[3], c, ahead_row(c, h))
    m1 = m - (em - behind_col(em, eh)) - (nm - behind_row(nm, nv))
    h1 = h - (eh - behind_col(eh, em)) - (nh - behind_row(nh, nc))
    v1 = v - (ev - behind_col(ev, ec)) - (nv - behind_row(nv, nm))
    v1 = jnp.where(inside > 0.0, v1, 0.0)
    em = flux(east[0], m1, ahead_col(m1, h1))
    eh = flux(east[1], h1, ahead_col(h1, m1))
    nm = flux(north[0], m1, ahead_row(m1, v1))
    nv = flux(north[2], v1, ahead_row(v1, m1))
    return m1 - (em - behind_col(em, eh)) - (nm - behind_row(nm, nv))


def pack_sides(tile, slot, packs):
    head, tail = packs
    lane = lane_id()
    here = (lane >= RIM * slot) & (lane < RIM * slot + RIM)
    head = jnp.where(here, pltpu.roll(tile, RIM * slot, 1), head)
    tail = jnp.where(here, pltpu.roll(tile, lax.rem(RIM * slot + RIM, COLS), 1), tail)
    return head, tail


def unpack_sides(from_right, from_left, slot):
    right = pltpu.roll(from_right, lax.rem(COLS - RIM * slot, COLS), 1)
    left = pltpu.roll(from_left, lax.rem(2 * COLS - RIM - RIM * slot, COLS), 1)
    return jnp.where(lane_id() < COLS // 2, right, left)


def tile_at(tile):
    return pl.ds(pl.multiple_of(tile * ROWS, ROWS), ROWS)


def kept_rows(edges):
    after = (row_id() == 0) & (edges[0] > 0)
    before = (row_id() == ROWS - 1) & (edges[1] > 0)
    return jnp.where(after | before, 1.0, 0.0)


def each_level(levels, step, carry, block):
    def trip(at, carry):
        for k in range(block):
            carry = step(block * at + k, carry)
        return carry

    return lax.fori_loop(0, levels // block, trip, carry)


def place(field, level, levels):
    per = SLOTS // levels
    return field // per, (field % per) * levels + level


def packed_tiles(fields, levels):
    return pl.cdiv(fields * levels, SLOTS)


def pack_fields(sources, levels, head_ref, tail_ref):
    count = packed_tiles(len(sources), levels)
    zero = jnp.zeros((ROWS, COLS), jnp.float32)

    def step(level, packs):
        packs = list(packs)
        for field, source in enumerate(sources):
            tile, slot = place(field, level, levels)
            packs[tile] = pack_sides(source(level), slot, packs[tile])
        return tuple(packs)

    packs = each_level(levels, step, ((zero, zero),) * count, 8)
    for tile, (head, tail) in enumerate(packs):
        head_ref[tile] = head
        tail_ref[tile] = tail


def pack_rows(sources, head, tail):
    at = 0
    total = sum(ref.shape[0] for ref in sources) // ROWS
    for ref in sources:
        tiles = ref.shape[0] // ROWS
        for row in range(RIM):
            head[pl.ds(row * total + at, tiles), :] = ref[pl.ds(row, tiles, stride=ROWS), :]
            tail[pl.ds(row * total + at, tiles), :] = ref[
                pl.ds(ROWS - RIM + row, tiles, stride=ROWS), :
            ]
        at += tiles


def row_payload(fields, levels):
    rows = RIM * fields * levels + 2 * RIM * packed_tiles(fields, levels)
    return -(-rows // 16) * 16


def pack_kernel(levels, tracers, winds, head, tail, head_rows, tail_rows):
    sources = []
    for ref in (tracers, winds):
        for f in range(ref.shape[0] // (levels * ROWS)):
            base = f * levels * ROWS
            sources.append(
                lambda level, ref=ref, base=base: ref[
                    pl.ds(pl.multiple_of(base + level * ROWS, ROWS), ROWS), :
                ]
            )
    pack_rows((tracers, winds), head_rows, tail_rows)
    pack_fields(sources, levels, head, tail)


def corner_kernel(head_in, tail_in, from_right, from_left, head, tail, near, far, sems):
    del head_in, tail_in
    near[...] = jnp.zeros(near.shape, jnp.float32)
    far[...] = jnp.zeros(far.shape, jnp.float32)
    at = 0
    for ref in (from_right, from_left):
        for tile in range(ref.shape[0]):
            near[at : at + RIM, :] = ref[tile, 0:RIM, :]
            far[at : at + RIM, :] = ref[tile, ROWS - RIM : ROWS, :]
            at += RIM
    base = head.shape[0] - near.shape[0]
    copies = [
        pltpu.make_async_copy(block, whole.at[pl.ds(base, near.shape[0])], sems.at[k])
        for k, (block, whole) in enumerate(((near, head), (far, tail)))
    ]
    for copy in copies:
        copy.start()
    for copy in copies:
        copy.wait()


def unpack_rows(from_north, from_south, rim_ref, corner_ref, tiles, packed):
    for row in range(RIM):
        rim_ref[pl.ds(row, tiles, stride=ROWS), :] = from_north[pl.ds(row * tiles, tiles), :]
        rim_ref[pl.ds(ROWS - RIM + row, tiles, stride=ROWS), :] = from_south[
            pl.ds(row * tiles, tiles), :
        ]
    at = RIM * tiles
    for tile in range(2 * packed):
        corner_ref[tile, 0:RIM, :] = from_north[at : at + RIM, :]
        corner_ref[tile, ROWS - RIM : ROWS, :] = from_south[at : at + RIM, :]
        at += RIM


def rim_tiles(field, level, levels, packed, right, left, rim_ref, corner_ref):
    tile, slot = place(field, level, levels)
    side = unpack_sides(right[tile], left[tile], slot)
    row = pl.multiple_of((field * levels + level) * ROWS, ROWS)
    rows = rim_ref[pl.ds(row, ROWS), :]
    corner = unpack_sides(corner_ref[tile], corner_ref[packed + tile], slot)
    return side, rows, corner


def first_kernel(
    tracers,
    winds,
    right,
    left,
    north,
    south,
    edges,
    gases,
    w1,
    b1,
    w2,
    b2,
    w3,
    lsolar,
    kappa,
    lground,
    scaled,
    state,
    heating,
    head,
    tail,
    head_rows,
    tail_rows,
    face,
    rim_ref,
    corner_ref,
    xs,
    hid_a,
    hid_b,
    hidden,
    logits,
    depth_a,
    depth_b,
    weight,
    sums,
):
    depths = (depth_a, depth_b)
    ntr, levels = tracers.shape[0], tracers.shape[1]
    fields = ntr + winds.shape[0]
    packed = packed_tiles(fields, levels)
    groups = lsolar.shape[0]
    hid = b1.shape[0]
    unpack_rows(north, south, rim_ref, corner_ref, fields * levels, packed)
    keep = kept_rows(edges)

    def transport(level, carry):
        rim = functools.partial(
            rim_tiles,
            level=level,
            levels=levels,
            packed=packed,
            right=right,
            left=left,
            rim_ref=rim_ref,
            corner_ref=corner_ref,
        )
        east, north_face = faces(
            (winds[0, level], *rim(ntr)), (winds[1, level], *rim(ntr + 1))
        )
        face[level] = jnp.stack([*east, *north_face])
        out = []
        for f in range(ntr):
            q = two_steps((tracers[f, level], *rim(f)), east, north_face, keep)
            state[tile_at(f * levels + level), :] = q
            out.append(q)
        xs[level] = jnp.concatenate(out, 0).astype(jnp.bfloat16)
        return carry

    each_level(levels, transport, 0, 4)

    diffuse = diffuse_factor * tau_scale
    pairs = levels // 2
    depths[0][0] = jnp.zeros((groups, ROWS, COLS), jnp.float32)
    depths[1][0] = jnp.zeros((groups, ROWS, COLS), jnp.float32)
    ones = jnp.ones((w3.shape[1] - hid, 2 * COLS), jnp.bfloat16)

    def silu(half):
        return (half + half * jnp.tanh(half)).astype(jnp.bfloat16)

    def layer_one(pair, out):
        x = jnp.concatenate(
            [jnp.concatenate([gases[2 * pair + k], xs[2 * pair + k]], 0) for k in range(2)], 1
        )
        wide = jnp.concatenate([b1[...]] * 2, 1)
        part = ROWS // 2
        for at in range(0, ROWS, part):
            mine = w1[at * hid : (at + part) * hid, :]
            y = jnp.dot(mine, x, preferred_element_type=jnp.float32)
            for k in range(part):
                out[(at + k) * hid : (at + k + 1) * hid, :] = silu(
                    y[k * hid : (k + 1) * hid] + wide
                )

    def layer_two(pair, source, at=lambda row, pair: row * pairs + pair):
        wide = jnp.concatenate([b2[...]] * 2, 1)
        for row in range(ROWS):
            y = source[row * hid : (row + 1) * hid, :]
            y = silu(jnp.dot(w2[...], y, preferred_element_type=jnp.float32) + wide)
            hidden[at(row, pair)] = jnp.concatenate([y, ones], 0)

    def layers(step, carry):
        layer_one(2 * step, hid_a)

        layer_two(
            2 * step - 1,
            hid_b,
            lambda row, pair: jnp.where(step == 0, ROWS * pairs, row * pairs + pair),
        )

        layer_one(2 * step + 1, hid_b)
        layer_two(2 * step, hid_a)
        return carry

    lax.fori_loop(0, pairs // 2, layers, 0)
    layer_two(pairs - 1, hid_b)

    def third(at):
        logits[...] = jnp.dot(w3[...], hidden[at], preferred_element_type=jnp.float32).reshape(
            groups, ROWS, 2 * COLS
        )

    def optical(pair, depth):
        t = logits[...] * log2e
        soft = jnp.maximum(t, jnp.log2(1.0 + jnp.exp2(jnp.minimum(t, 126.0))))
        d = depth[2 * pair] + soft[:, :, :COLS]
        depth[2 * pair + 1] = d
        depth[2 * pair + 2] = d + soft[:, :, COLS:]

    def light(row, level, depth):
        d = depth[level]
        direct = jnp.exp2(lsolar[...] - d * kappa[row][None])
        upward = jnp.exp2(weight[...] + d * diffuse)
        sums[row, level] = jnp.sum(direct - upward, 0)

    def close(row, depth):
        total = depth[levels]
        weight[...] = (
            lsolar[...] + lground[row][None] - total * (kappa[row] + diffuse)[None]
        )
        light(row, levels, depth)

    def both(row, depth, before):
        close(row - 1, before)

        def step(pair, carry):
            optical(pair, depth)
            light(row - 1, 2 * pair, before)
            light(row - 1, 2 * pair + 1, before)
            third(row * pairs + pair + 1)
            return carry

        lax.fori_loop(0, pairs, step, 0)

    def only_optical(pair, carry):
        optical(pair, depths[0])
        third(pair + 1)
        return carry

    third(0)
    lax.fori_loop(0, pairs, only_optical, 0)

    def two_rows(step, carry):
        both(2 * step + 1, depths[1], depths[0])
        both(2 * step + 2, depths[0], depths[1])
        return carry

    lax.fori_loop(0, ROWS // 2 - 1, two_rows, 0)
    both(ROWS - 1, depths[1], depths[0])
    close(ROWS - 1, depths[1])

    def only_light(pair, carry):
        light(ROWS - 1, 2 * pair, depths[1])
        light(ROWS - 1, 2 * pair + 1, depths[1])
        return carry

    lax.fori_loop(0, pairs, only_light, 0)

    for row in range(ROWS):
        change = sums[row, 0:levels] - sums[row, 1 : levels + 1]
        heating[:, row, :] = jnp.sum(change, 1) * scaled[row : row + 1, :]

    def add(level, carry):
        tile = tile_at(level)
        state[tile, :] = state[tile, :] + heating[level]
        return carry

    each_level(levels, add, 0, 8)
    pack_rows((state,), head_rows, tail_rows)
    pack_fields(
        [lambda level, f=f: state[tile_at(f * levels + level), :] for f in range(ntr)],
        levels,
        head,
        tail,
    )


def last_kernel(tracers, face, right, left, north, south, edges, out, rim_ref, corner_ref):
    ntr, levels = out.shape[0], out.shape[1]
    packed = packed_tiles(ntr, levels)
    unpack_rows(north, south, rim_ref, corner_ref, ntr * levels, packed)
    keep = kept_rows(edges)

    def transport(level, carry):
        rim = functools.partial(
            rim_tiles,
            level=level,
            levels=levels,
            packed=packed,
            right=right,
            left=left,
            rim_ref=rim_ref,
            corner_ref=corner_ref,
        )
        tiles = [face[level, k] for k in range(8)]
        for f in range(ntr):
            q = tracers[tile_at(f * levels + level), :]
            out[f, level] = two_steps((q, *rim(f)), tiles[:4], tiles[4:], keep)
        return carry

    each_level(levels, transport, 0, 4)


def prepare_kernel(
    index,
    slot,
    ground,
    table,
    solar,
    w_first,
    b_first,
    w_second,
    b_second,
    w_third,
    b_third,
    w1,
    b1,
    w2,
    b2,
    w3,
    lsolar,
    kappa,
    lground,
    scaled,
    square,
    wide,
):
    feat, hid = w_first.shape
    bands = solar.shape[1]

    def column(ref, factor):
        square[:, 0 : ref.shape[1]] = jnp.broadcast_to(ref[...], (COLS, ref.shape[1])) * factor
        return jnp.transpose(square[...])[0 : ref.shape[1]]

    square[...] = jnp.zeros(square.shape, jnp.float32)
    b1[...] = column(b_first, 0.5)
    b2[...] = column(b_second, 0.5)

    square[...] = jnp.zeros(square.shape, jnp.float32)
    square[0:hid, 0:hid] = w_second[...].astype(jnp.float32) * 0.5
    w2[...] = jnp.transpose(square[...])[0:hid, 0:hid].astype(jnp.bfloat16)

    square[...] = jnp.zeros(square.shape, jnp.float32)
    square[0:feat, 0:hid] = w_first[...].astype(jnp.float32) * 0.5
    by_unit = jnp.transpose(square[...])[0:hid].astype(jnp.bfloat16)
    source = lax.broadcasted_iota(jnp.int32, (COLS, COLS), 0)
    lane = lax.broadcasted_iota(jnp.int32, (COLS, COLS), 1)
    spread = jnp.where(lane // ROWS == source, 1.0, 0.0).astype(jnp.bfloat16)
    by_lane = jnp.dot(by_unit, spread, preferred_element_type=jnp.float32)
    of_row = lax.broadcasted_iota(jnp.int32, (hid, COLS), 1) % ROWS
    for row in range(ROWS):
        w1[row * hid : (row + 1) * hid, :] = jnp.where(of_row == row, by_lane, 0.0).astype(
            jnp.bfloat16
        )

    wide[...] = jnp.zeros(wide.shape, jnp.float32)
    wide[0:hid, 0:bands] = w_third[...].astype(jnp.float32)
    rest = b_third[...]
    for k in range(3):
        part = rest.astype(jnp.bfloat16).astype(jnp.float32)
        wide[hid + k : hid + k + 1, 0:bands] = part
        rest = rest - part
    w3[...] = jnp.transpose(wide[...])[0:bands, 0 : w3.shape[1]].astype(jnp.bfloat16)

    wide[:, 0:bands] = jnp.broadcast_to(jnp.log2(solar[...]), (COLS, bands))
    lsolar[...] = jnp.transpose(wide[...])[0:bands].reshape(lsolar.shape)

    ids = index[...]
    cosine = jnp.zeros((ROWS, COLS), jnp.float32)
    for entry in range(1, table.shape[0]):
        cosine = jnp.where(ids == entry, table[entry], cosine)
    slant = tau_scale / jnp.maximum(cosine, mu_floor)
    lg = jnp.log2(ground[...].astype(jnp.float32))
    for row in range(ROWS):
        kappa[row] = jnp.broadcast_to(slant[row : row + 1], (ROWS, COLS))
        lground[row] = jnp.broadcast_to(lg[row : row + 1], (ROWS, COLS))
        lit = jnp.where(slot[0, row] >= 0, heat_scale, 0.0)
        scaled[row : row + 1, :] = lit * cosine[row : row + 1]


vmem = pl.BlockSpec(memory_space=pltpu.VMEM)
smem = pl.BlockSpec(memory_space=pltpu.SMEM)
f32 = jnp.float32


def tiles_like(*shape):
    return jax.ShapeDtypeStruct(shape, f32)


def shift(x, axis, by, wrap):
    count = lax.axis_size(axis)
    return lax.ppermute(
        x, axis, [(i, (i + by) % count) for i in range(count) if wrap or 0 <= i + by < count]
    )


def exchange_cols(head, tail):
    return shift(head, "lon", -1, True), shift(tail, "lon", 1, True)


def exchange_rows(head, tail, right, left):
    any_space = pl.BlockSpec(memory_space=pl.ANY)
    spare = -(-2 * RIM * right.shape[0] // 16) * 16
    head, tail = pl.pallas_call(
        corner_kernel,
        in_specs=[any_space] * 2 + [vmem] * 2,
        out_specs=[any_space] * 2,
        out_shape=[tiles_like(*head.shape)] * 2,
        input_output_aliases={0: 0, 1: 1},
        scratch_shapes=[pltpu.VMEM((spare, COLS), f32)] * 2 + [pltpu.SemaphoreType.DMA((2,))],
        name="add_corners",
    )(head, tail, right, left)
    return shift(head, "lat", -1, False), shift(tail, "lat", 1, False)


def body(
    tracers,
    winds,
    gases,
    sun_index,
    block_slot,
    albedo,
    sun_table,
    solar,
    w_first,
    b_first,
    w_second,
    b_second,
    w_third,
    b_third,
):
    ntr, levels, clat, width = tracers.shape
    fields = ntr + winds.shape[0]
    gas = gases.shape[0]
    hid = w_first.shape[1]
    bands = solar.shape[0]
    if (clat, width) != (ROWS, COLS) or w_first.shape[0] * ROWS != COLS or levels % 8 or SLOTS % levels or bands % ROWS:
        raise ValueError("unsupported sizes")

    flat = (tracers.reshape(-1, COLS), winds.reshape(-1, COLS))
    columns = tiles_like(packed_tiles(fields, levels), ROWS, COLS)
    head, tail, head_rows, tail_rows = pl.pallas_call(
        functools.partial(pack_kernel, levels),
        in_specs=[vmem] * 2,
        out_specs=[vmem] * 4,
        out_shape=[columns] * 2 + [tiles_like(row_payload(fields, levels), COLS)] * 2,
        name="pack",
    )(*flat)
    right, left = exchange_cols(head, tail)

    groups = bands // ROWS
    bf16 = jnp.bfloat16
    prepared = pl.pallas_call(
        prepare_kernel,
        in_specs=[vmem, smem, vmem, smem] + [vmem] * 7,
        out_specs=[vmem] * 9,
        out_shape=[
            jax.ShapeDtypeStruct((ROWS * hid, w_first.shape[0] * ROWS), bf16),
            tiles_like(hid, COLS),
            jax.ShapeDtypeStruct((hid, hid), bf16),
            tiles_like(hid, COLS),
            jax.ShapeDtypeStruct((bands, hid + 16), bf16),
            tiles_like(groups, ROWS, COLS),
            tiles_like(ROWS, ROWS, COLS),
            tiles_like(ROWS, ROWS, COLS),
            tiles_like(ROWS, COLS),
        ],
        scratch_shapes=[
            pltpu.VMEM((COLS, COLS), f32),
            pltpu.VMEM((COLS, pl.cdiv(bands, COLS) * COLS), f32),
        ],
        name="prepare",
    )(
        sun_index,
        block_slot.reshape(1, -1),
        albedo,
        sun_table,
        solar.reshape(1, -1),
        w_first,
        b_first.reshape(1, -1),
        w_second,
        b_second.reshape(1, -1),
        w_third,
        b_third.reshape(1, -1),
    )
    gas_rows = gases.transpose(1, 0, 2, 3).reshape(levels, gas * ROWS, COLS)
    lat = lax.axis_index("lat")
    edges = jnp.stack([lat < lax.axis_size("lat") - 1, lat > 0]).astype(jnp.int32)
    right, left, prepared, gas_rows = lax.optimization_barrier((right, left, prepared, gas_rows))
    north, south = exchange_rows(head_rows, tail_rows, right, left)

    packed = packed_tiles(fields, levels)
    state, heating, head, tail, head_rows, tail_rows, face = pl.pallas_call(
        first_kernel,
        in_specs=[vmem] * 6 + [smem] + [vmem] * 10,
        out_specs=[vmem] * 7,
        out_shape=[
            tiles_like(ntr * levels * ROWS, COLS),
            tiles_like(levels, ROWS, COLS),
        ]
        + [tiles_like(packed_tiles(ntr, levels), ROWS, COLS)] * 2
        + [tiles_like(row_payload(ntr, levels), COLS)] * 2
        + [tiles_like(levels, 8, ROWS, COLS)],
        scratch_shapes=[
            pltpu.VMEM((fields * levels * ROWS, COLS), f32),
            pltpu.VMEM((2 * packed, ROWS, COLS), f32),
            pltpu.VMEM((levels, ntr * ROWS, COLS), bf16),
            pltpu.VMEM((ROWS * hid, 2 * COLS), bf16),
            pltpu.VMEM((ROWS * hid, 2 * COLS), bf16),
            pltpu.VMEM((ROWS * levels // 2 + 1, hid + 16, 2 * COLS), bf16),
            pltpu.VMEM((groups, ROWS, 2 * COLS), f32),
            pltpu.VMEM((levels + 1, groups, ROWS, COLS), f32),
            pltpu.VMEM((levels + 1, groups, ROWS, COLS), f32),
            pltpu.VMEM((groups, ROWS, COLS), f32),
            pltpu.VMEM((ROWS, levels + 1, ROWS, COLS), f32),
        ],
        name="transport_radiation",
    )(tracers, winds, right, left, north, south, edges, gas_rows, *prepared)

    right, left = exchange_cols(head, tail)
    north, south = exchange_rows(head_rows, tail_rows, right, left)
    final = pl.pallas_call(
        last_kernel,
        in_specs=[vmem] * 6 + [smem],
        out_specs=vmem,
        out_shape=tiles_like(ntr, levels, ROWS, COLS),
        scratch_shapes=[
            pltpu.VMEM((ntr * levels * ROWS, COLS), f32),
            pltpu.VMEM((2 * packed_tiles(ntr, levels), ROWS, COLS), f32),
        ],
        name="last_transport",
    )(state, face, right, left, north, south, edges)
    return final, heating


def solution(mesh):
    grid = P(None, None, "lat", "lon")
    in_specs = (grid, grid, grid) + (P("lat", "lon"),) * 3 + (P(),) * 8
    out_specs = (grid, P(None, "lat", "lon"))
    return jax.shard_map(body, mesh=mesh, in_specs=in_specs, out_specs=out_specs, check_vma=False)
```

```python
import functools
import math

import jax
import jax.numpy as jnp
from jax import lax
from jax.experimental import pallas as pl
from jax.experimental.pallas import tpu as pltpu
from jax.sharding import PartitionSpec as P

tau_scale = 0.05
mu_floor = 0.05
heat_scale = 30.0
diffuse_factor = 1.66
log2e = 1.4426950408889634

ROWS = 8
COLS = 128
RIM = 2
SLOTS = COLS // RIM
HAS_AFTER, HAS_BEFORE, LAT_EVEN, LON_EVEN = range(4)


def lane_id():
    return lax.broadcasted_iota(jnp.int32, (ROWS, COLS), 1)


def row_id():
    return lax.broadcasted_iota(jnp.int32, (ROWS, COLS), 0)


def ahead_row(tile, beside):
    return pltpu.roll(jnp.where(row_id() == 0, beside, tile), ROWS - 1, 0)


def behind_row(tile, beside):
    return pltpu.roll(jnp.where(row_id() == ROWS - 1, beside, tile), 1, 0)


def flux(face, here, there):
    return jnp.maximum(face, 0.0) * here + jnp.minimum(face, 0.0) * there


def next_col(tile, rim):
    return jnp.where(lane_id() == COLS - 1, rim, pltpu.roll(tile, COLS - 1, 1))


def col_change(face, first, tile, rim):
    out = flux(face, tile, next_col(tile, rim))
    return out - jnp.where(lane_id() == 0, flux(first, rim, tile), pltpu.roll(out, 1, 1))


def col_faces(wind, rim):
    return 0.5 * (wind + next_col(wind, rim)), 0.5 * (rim + wind)


def row_faces(main, rows):
    return 0.5 * (main + ahead_row(main, rows)), 0.5 * (rows + ahead_row(rows, main))


def row_changes(face, main, rows):
    out = flux(face[0], main, ahead_row(main, rows))
    rim = flux(face[1], rows, ahead_row(rows, main))
    return out - behind_row(out, rim), rim - behind_row(rim, out)


def two_steps(main, rows, side, corner, next_side, face, inside):
    north, south = row_changes(face[4:], main, rows)
    main1 = main - col_change(face[0], face[1], main, side) - north
    rows1 = rows - col_change(face[2], face[3], rows, corner) - south
    rows1 = jnp.where(inside > 0.0, rows1, 0.0)
    north, _ = row_changes(face[4:], main1, rows1)
    return main1 - col_change(face[0], face[1], main1, next_side) - north


def pack_sides(tile, slot, packs):
    head, tail = packs
    lane = lane_id()
    here = (lane >= RIM * slot) & (lane < RIM * slot + RIM)
    head = jnp.where(here, pltpu.roll(tile, RIM * slot, 1), head)
    tail = jnp.where(here, pltpu.roll(tile, lax.rem(RIM * slot + RIM, COLS), 1), tail)
    return head, tail


def tile_at(tile):
    return pl.ds(pl.multiple_of(tile * ROWS, ROWS), ROWS)


def kept_rows(flags):
    after = (row_id() == 0) & (flags[HAS_AFTER] > 0)
    before = (row_id() == ROWS - 1) & (flags[HAS_BEFORE] > 0)
    return jnp.where(after | before, 1.0, 0.0)


def each_level(levels, step, carry, block):
    def trip(at, carry):
        for k in range(block):
            carry = step(block * at + k, carry)
        return carry

    return lax.fori_loop(0, levels // block, trip, carry)


def place(field, level, levels):
    per = SLOTS // levels
    return field // per, (field % per) * levels + level


def packed_tiles(fields, levels):
    return pl.cdiv(fields * levels, SLOTS)


def pack_fields(sources, levels, even, one_ref, two_ref):
    count = packed_tiles(len(sources), levels)
    zero = jnp.zeros((ROWS, COLS), jnp.float32)

    def step(level, packs):
        packs = list(packs)
        for field, source in enumerate(sources):
            tile, slot = place(field, level, levels)
            packs[tile] = pack_sides(source(level), slot, packs[tile])
        return tuple(packs)

    packs = each_level(levels, step, ((zero, zero),) * count, 8)
    for tile, (head, tail) in enumerate(packs):
        one_ref[tile] = jnp.where(even, tail, head)
        two_ref[tile] = jnp.where(even, head, tail)


def pack_rows(sources, even, one, two):
    at = 0
    total = sum(ref.shape[0] for ref in sources) // ROWS
    for ref in sources:
        tiles = ref.shape[0] // ROWS
        for row in range(RIM):
            head = ref[pl.ds(row, tiles, stride=ROWS), :]
            tail = ref[pl.ds(ROWS - RIM + row, tiles, stride=ROWS), :]
            one[pl.ds(row * total + at, tiles), :] = jnp.where(even, tail, head)
            two[pl.ds(row * total + at, tiles), :] = jnp.where(even, head, tail)
        at += tiles


def row_payload(fields, levels):
    rows = RIM * fields * levels + 2 * RIM * packed_tiles(fields, levels)
    return -(-rows // 16) * 16


def pack_kernel(levels, flags, tracers, winds, one, two, one_rows, two_rows):
    sources = []
    for ref in (tracers, winds):
        for f in range(ref.shape[0] // (levels * ROWS)):
            base = f * levels * ROWS
            sources.append(
                lambda level, ref=ref, base=base: ref[
                    pl.ds(pl.multiple_of(base + level * ROWS, ROWS), ROWS), :
                ]
            )
    pack_rows((tracers, winds), flags[LAT_EVEN] > 0, one_rows, two_rows)
    pack_fields(sources, levels, flags[LON_EVEN] > 0, one, two)


def in_order(even, one, two):
    return jnp.where(even, one, two), jnp.where(even, two, one)


def corner_kernel(one_in, two_in, flags, cols_one, cols_two, one, two, near, far, sems):
    del one_in, two_in
    near[...] = jnp.zeros(near.shape, jnp.float32)
    far[...] = jnp.zeros(far.shape, jnp.float32)
    lon_even, lat_even = flags[LON_EVEN] > 0, flags[LAT_EVEN] > 0
    count = cols_one.shape[0]
    for tile in range(count):
        for side, block in enumerate(in_order(lon_even, cols_one[tile], cols_two[tile])):
            at = RIM * (side * count + tile)
            head, tail = block[0:RIM], block[ROWS - RIM : ROWS]
            near[at : at + RIM, :] = jnp.where(lat_even, tail, head)
            far[at : at + RIM, :] = jnp.where(lat_even, head, tail)
    base = one.shape[0] - near.shape[0]
    copies = [
        pltpu.make_async_copy(block, whole.at[pl.ds(base, near.shape[0])], sems.at[k])
        for k, (block, whole) in enumerate(((near, one), (far, two)))
    ]
    for copy in copies:
        copy.start()
    for copy in copies:
        copy.wait()


def unpack_rows(even, rows_one, rows_two, rim_ref, corner_ref, tiles, packed):
    for row in range(RIM):
        here = pl.ds(row * tiles, tiles)
        after, before = in_order(even, rows_one[here, :], rows_two[here, :])
        rim_ref[pl.ds(row, tiles, stride=ROWS), :] = after
        rim_ref[pl.ds(ROWS - RIM + row, tiles, stride=ROWS), :] = before
    for tile in range(2 * packed):
        at = RIM * (tiles + tile)
        after, before = in_order(even, rows_one[at : at + RIM, :], rows_two[at : at + RIM, :])
        corner_ref[tile, 0:RIM, :] = after
        corner_ref[tile, ROWS - RIM : ROWS, :] = before


def paired(after, before):
    return jnp.where(lane_id() % 2 == 0, after, before)


def side_tiles(even, own_one, own_two, cols_one, cols_two, corner_ref, tile, packed):
    right, left = in_order(even, cols_one[tile], cols_two[tile])
    tail, head = in_order(even, own_one[tile], own_two[tile])
    return (
        paired(right, left),
        paired(pltpu.roll(right, COLS - 1, 1), pltpu.roll(head, 1, 1)),
        paired(pltpu.roll(tail, COLS - 1, 1), pltpu.roll(left, 1, 1)),
        paired(corner_ref[tile], corner_ref[packed + tile]),
    )


def side_faces(tiles):
    low = lane_id() < COLS // 2
    half = [pltpu.roll(t, COLS // 2, 1) for t in tiles]
    u, after, before, _ = [jnp.where(low, t, h) for t, h in zip(tiles, half)]
    v, _, _, corner = [jnp.where(low, h, t) for t, h in zip(tiles, half)]
    return (0.5 * (u + after), 0.5 * (before + u), *row_faces(v, corner))


def side_step(tiles, face):
    here, after, before, corner = tiles
    east = flux(face[0], here, after) - flux(face[1], before, here)
    return here - east - row_changes(face[2:], here, corner)[0]


def from_side(ref, field, level, levels):
    tile, slot = place(field, level, levels)
    return pltpu.roll(ref[tile], COLS - 1 - RIM * slot, 1)


def first_kernel(
    tracers,
    winds,
    own_one,
    own_two,
    cols_one,
    cols_two,
    rows_one,
    rows_two,
    flags,
    gases,
    w1,
    b1,
    w2,
    b2,
    w3,
    lsolar,
    kappa,
    lground,
    scaled,
    state,
    heating,
    next_one,
    next_two,
    next_rows_one,
    next_rows_two,
    face,
    side_face,
    rim_ref,
    corner_ref,
    side_ref,
    next_side_ref,
    side_rim_ref,
    xs,
    hid_a,
    hid_b,
    hidden,
    logits_a,
    logits_b,
    depth_a,
    depth_b,
    weight,
    sums,
):
    depths = (depth_a, depth_b)
    ntr, levels = tracers.shape[0], tracers.shape[1]
    fields = ntr + winds.shape[0]
    packed = packed_tiles(fields, levels)
    groups = lsolar.shape[0]
    hid = b1.shape[0]
    lon_even, lat_even = flags[LON_EVEN] > 0, flags[LAT_EVEN] > 0
    unpack_rows(lat_even, rows_one, rows_two, rim_ref, corner_ref, fields * levels, packed)
    keep = kept_rows(flags)
    sides = [
        side_tiles(lon_even, own_one, own_two, cols_one, cols_two, corner_ref, tile, packed)
        for tile in range(packed)
    ]
    of_sides = side_faces(sides[packed - 1])
    for k, tile in enumerate(of_sides):
        side_face[k] = tile
    for tile in range(packed):
        side_ref[tile] = sides[tile][0]
        side_rim_ref[tile] = sides[tile][3]
        if tile < packed - 1:
            next_side_ref[tile] = side_step(sides[tile], of_sides)

    def transport(level, carry):
        def rows_of(field):
            return rim_ref[tile_at(field * levels + level), :]

        tiles = (
            *col_faces(winds[0, level], from_side(side_ref, ntr, level, levels)),
            *col_faces(rows_of(ntr), from_side(side_rim_ref, ntr, level, levels)),
            *row_faces(winds[1, level], rows_of(ntr + 1)),
        )
        for k, tile in enumerate(tiles):
            face[level, k] = tile
        out = []
        for f in range(ntr):
            q = two_steps(
                tracers[f, level],
                rows_of(f),
                from_side(side_ref, f, level, levels),
                from_side(side_rim_ref, f, level, levels),
                from_side(next_side_ref, f, level, levels),
                tiles,
                keep,
            )
            state[tile_at(f * levels + level), :] = q
            out.append(q)
        xs[level] = jnp.concatenate(out, 0).astype(jnp.bfloat16)
        return carry

    each_level(levels, transport, 0, 4)

    diffuse = diffuse_factor * tau_scale
    pairs = levels // 2
    depths[0][0] = jnp.zeros((groups, ROWS, COLS), jnp.float32)
    depths[1][0] = jnp.zeros((groups, ROWS, COLS), jnp.float32)
    ones = jnp.ones((w3.shape[1] - hid, 2 * COLS), jnp.bfloat16)

    def silu(half):
        return (half + half * jnp.tanh(half)).astype(jnp.bfloat16)

    def layer_one(pair, out):
        x = jnp.concatenate(
            [jnp.concatenate([gases[2 * pair + k], xs[2 * pair + k]], 0) for k in range(2)], 1
        )
        wide = jnp.concatenate([b1[...]] * 2, 1)
        part = ROWS // 2
        for at in range(0, ROWS, part):
            mine = w1[at * hid : (at + part) * hid, :]
            y = jnp.dot(mine, x, preferred_element_type=jnp.float32)
            for k in range(part):
                out[(at + k) * hid : (at + k + 1) * hid, :] = silu(
                    y[k * hid : (k + 1) * hid] + wide
                )

    def layer_two(pair, source, at=lambda row, pair: row * pairs + pair):
        wide = jnp.concatenate([b2[...]] * 2, 1)
        for row in range(ROWS):
            y = source[row * hid : (row + 1) * hid, :]
            y = silu(jnp.dot(w2[...], y, preferred_element_type=jnp.float32) + wide)
            hidden[at(row, pair)] = jnp.concatenate([y, ones], 0)

    def layers(step, carry):
        layer_one(2 * step, hid_a)

        layer_two(
            2 * step - 1,
            hid_b,
            lambda row, pair: jnp.where(step == 0, ROWS * pairs, row * pairs + pair),
        )

        layer_one(2 * step + 1, hid_b)
        layer_two(2 * step, hid_a)
        return carry

    lax.fori_loop(0, pairs // 2, layers, 0)
    layer_two(pairs - 1, hid_b)

    def third(at, buf):
        buf[...] = jnp.dot(w3[...], hidden[at], preferred_element_type=jnp.float32).reshape(
            groups, ROWS, 2 * COLS
        )

    def optical(pair, depth, buf):
        t = buf[...] * log2e
        soft = jnp.maximum(t, jnp.log2(1.0 + jnp.exp2(jnp.minimum(t, 126.0))))
        d = depth[2 * pair] + soft[:, :, :COLS]
        depth[2 * pair + 1] = d
        depth[2 * pair + 2] = d + soft[:, :, COLS:]

    def light(row, level, depth):
        d = depth[level]
        direct = jnp.exp2(lsolar[...] - d * kappa[row][None])
        upward = jnp.exp2(weight[...] + d * diffuse)
        sums[row, level] = jnp.sum(direct - upward, 0)

    def close(row, depth):
        total = depth[levels]
        weight[...] = (
            lsolar[...] + lground[row][None] - total * (kappa[row] + diffuse)[None]
        )
        light(row, levels, depth)

    def both(row, depth, before):
        close(row - 1, before)

        def step(trip, carry):
            for k, buf in enumerate(bufs):
                pair = 2 * trip + k
                optical(pair, depth, buf)
                light(row - 1, 2 * pair, before)
                light(row - 1, 2 * pair + 1, before)
                third(row * pairs + pair + 2, buf)
            return carry

        lax.fori_loop(0, pairs // 2, step, 0)

    def only_optical(trip, carry):
        for k, buf in enumerate(bufs):
            optical(2 * trip + k, depths[0], buf)
            third(2 * trip + k + 2, buf)
        return carry

    bufs = (logits_a, logits_b)
    third(0, logits_a)
    third(1, logits_b)
    lax.fori_loop(0, pairs // 2, only_optical, 0)

    def two_rows(step, carry):
        both(2 * step + 1, depths[1], depths[0])
        both(2 * step + 2, depths[0], depths[1])
        return carry

    lax.fori_loop(0, ROWS // 2 - 1, two_rows, 0)
    both(ROWS - 1, depths[1], depths[0])
    close(ROWS - 1, depths[1])

    def only_light(pair, carry):
        light(ROWS - 1, 2 * pair, depths[1])
        light(ROWS - 1, 2 * pair + 1, depths[1])
        return carry

    lax.fori_loop(0, pairs, only_light, 0)

    for row in range(ROWS):
        change = sums[row, 0:levels] - sums[row, 1 : levels + 1]
        heating[:, row, :] = jnp.sum(change, 1) * scaled[row : row + 1, :]

    def add(level, carry):
        tile = tile_at(level)
        state[tile, :] = state[tile, :] + heating[level]
        return carry

    each_level(levels, add, 0, 8)
    pack_rows((state,), lat_even, next_rows_one, next_rows_two)
    pack_fields(
        [lambda level, f=f: state[tile_at(f * levels + level), :] for f in range(ntr)],
        levels,
        lon_even,
        next_one,
        next_two,
    )


def last_kernel(
    tracers,
    face,
    side_face,
    own_one,
    own_two,
    cols_one,
    cols_two,
    rows_one,
    rows_two,
    flags,
    out,
    rim_ref,
    corner_ref,
    side_ref,
    next_side_ref,
    side_rim_ref,
):
    ntr, levels = out.shape[0], out.shape[1]
    packed = packed_tiles(ntr, levels)
    lon_even, lat_even = flags[LON_EVEN] > 0, flags[LAT_EVEN] > 0
    unpack_rows(lat_even, rows_one, rows_two, rim_ref, corner_ref, ntr * levels, packed)
    keep = kept_rows(flags)
    of_sides = [side_face[k] for k in range(4)]
    for tile in range(packed):
        sides = side_tiles(
            lon_even, own_one, own_two, cols_one, cols_two, corner_ref, tile, packed
        )
        side_ref[tile] = sides[0]
        side_rim_ref[tile] = sides[3]
        next_side_ref[tile] = side_step(sides, of_sides)

    def transport(level, carry):
        tiles = [face[level, k] for k in range(6)]
        for f in range(ntr):
            out[f, level] = two_steps(
                tracers[tile_at(f * levels + level), :],
                rim_ref[tile_at(f * levels + level), :],
                from_side(side_ref, f, level, levels),
                from_side(side_rim_ref, f, level, levels),
                from_side(next_side_ref, f, level, levels),
                tiles,
                keep,
            )
        return carry

    each_level(levels, transport, 0, 4)


def prepare_kernel(
    index,
    slot,
    ground,
    table,
    solar,
    w_first,
    b_first,
    w_second,
    b_second,
    w_third,
    b_third,
    w1,
    b1,
    w2,
    b2,
    w3,
    lsolar,
    kappa,
    lground,
    scaled,
    square,
    wide,
):
    feat, hid = w_first.shape
    bands = solar.shape[1]

    def column(ref, factor):
        square[:, 0 : ref.shape[1]] = jnp.broadcast_to(ref[...], (COLS, ref.shape[1])) * factor
        return jnp.transpose(square[...])[0 : ref.shape[1]]

    square[...] = jnp.zeros(square.shape, jnp.float32)
    b1[...] = column(b_first, 0.5)
    b2[...] = column(b_second, 0.5)

    square[...] = jnp.zeros(square.shape, jnp.float32)
    square[0:hid, 0:hid] = w_second[...].astype(jnp.float32) * 0.5
    w2[...] = jnp.transpose(square[...])[0:hid, 0:hid].astype(jnp.bfloat16)

    square[...] = jnp.zeros(square.shape, jnp.float32)
    square[0:feat, 0:hid] = w_first[...].astype(jnp.float32) * 0.5
    by_unit = jnp.transpose(square[...])[0:hid].astype(jnp.bfloat16)
    source = lax.broadcasted_iota(jnp.int32, (COLS, COLS), 0)
    lane = lax.broadcasted_iota(jnp.int32, (COLS, COLS), 1)
    spread = jnp.where(lane // ROWS == source, 1.0, 0.0).astype(jnp.bfloat16)
    by_lane = jnp.dot(by_unit, spread, preferred_element_type=jnp.float32)
    of_row = lax.broadcasted_iota(jnp.int32, (hid, COLS), 1) % ROWS
    for row in range(ROWS):
        w1[row * hid : (row + 1) * hid, :] = jnp.where(of_row == row, by_lane, 0.0).astype(
            jnp.bfloat16
        )

    wide[...] = jnp.zeros(wide.shape, jnp.float32)
    wide[0:hid, 0:bands] = w_third[...].astype(jnp.float32)
    rest = b_third[...]
    for k in range(3):
        part = rest.astype(jnp.bfloat16).astype(jnp.float32)
        wide[hid + k : hid + k + 1, 0:bands] = part
        rest = rest - part
    w3[...] = jnp.transpose(wide[...])[0:bands, 0 : w3.shape[1]].astype(jnp.bfloat16)

    wide[:, 0:bands] = jnp.broadcast_to(jnp.log2(solar[...]), (COLS, bands))
    lsolar[...] = jnp.transpose(wide[...])[0:bands].reshape(lsolar.shape)

    ids = index[...]
    cosine = jnp.zeros((ROWS, COLS), jnp.float32)
    for entry in range(1, table.shape[0]):
        cosine = jnp.where(ids == entry, table[entry], cosine)
    slant = tau_scale / jnp.maximum(cosine, mu_floor)
    lg = jnp.log2(ground[...].astype(jnp.float32))
    for row in range(ROWS):
        kappa[row] = jnp.broadcast_to(slant[row : row + 1], (ROWS, COLS))
        lground[row] = jnp.broadcast_to(lg[row : row + 1], (ROWS, COLS))
        lit = jnp.where(slot[0, row] >= 0, heat_scale, 0.0)
        scaled[row : row + 1, :] = lit * cosine[row : row + 1]


vmem = pl.BlockSpec(memory_space=pltpu.VMEM)
smem = pl.BlockSpec(memory_space=pltpu.SMEM)
f32 = jnp.float32


def tiles_like(*shape):
    return jax.ShapeDtypeStruct(shape, f32)


def swap_pairs(one, two, axis, ring):
    count = lax.axis_size(axis)
    near = [(i, i ^ 1) for i in range(count)]
    far = [(i, (i - 1 if i % 2 == 0 else i + 1) % count) for i in range(count)]
    if not ring:
        far = [(i, j) for i, j in far if abs(i - j) == 1]
    return lax.ppermute(one, axis, near), lax.ppermute(two, axis, far)


def exchange_rows(one, two, flags, cols):
    any_space = pl.BlockSpec(memory_space=pl.ANY)
    spare = -(-2 * RIM * cols[0].shape[0] // 16) * 16
    one, two = pl.pallas_call(
        corner_kernel,
        in_specs=[any_space] * 2 + [smem] + [vmem] * 2,
        out_specs=[any_space] * 2,
        out_shape=[tiles_like(*one.shape)] * 2,
        input_output_aliases={0: 0, 1: 1},
        scratch_shapes=[pltpu.VMEM((spare, COLS), f32)] * 2 + [pltpu.SemaphoreType.DMA((2,))],
        name="add_corners",
    )(one, two, flags, *cols)
    return swap_pairs(one, two, "lat", False)


def body(
    tracers,
    winds,
    gases,
    sun_index,
    block_slot,
    albedo,
    sun_table,
    solar,
    w_first,
    b_first,
    w_second,
    b_second,
    w_third,
    b_third,
):
    ntr, levels, clat, width = tracers.shape
    fields = ntr + winds.shape[0]
    gas = gases.shape[0]
    hid = w_first.shape[1]
    bands = solar.shape[0]
    if lax.axis_size("lat") % 2 or lax.axis_size("lon") % 2:
        raise ValueError("unsupported mesh")
    if (clat, width) != (ROWS, COLS) or w_first.shape[0] * ROWS != COLS or levels % 8 or 2 * levels != SLOTS or ntr % 2 or SLOTS % levels or bands % ROWS:
        raise ValueError("unsupported sizes")

    flat = (tracers.reshape(-1, COLS), winds.reshape(-1, COLS))
    columns = tiles_like(packed_tiles(fields, levels), ROWS, COLS)
    lat, lats = lax.axis_index("lat"), lax.axis_size("lat")
    flags = [lat < lats - 1, lat > 0, lat % 2 == 0, lax.axis_index("lon") % 2 == 0]
    flags = jnp.stack(flags).astype(jnp.int32)
    one, two, rows_one, rows_two = pl.pallas_call(
        functools.partial(pack_kernel, levels),
        in_specs=[smem] + [vmem] * 2,
        out_specs=[vmem] * 4,
        out_shape=[columns] * 2 + [tiles_like(row_payload(fields, levels), COLS)] * 2,
        name="pack",
    )(flags, *flat)
    own = (one, two)
    cols = swap_pairs(one, two, "lon", True)

    groups = bands // ROWS
    bf16 = jnp.bfloat16
    prepared = pl.pallas_call(
        prepare_kernel,
        in_specs=[vmem, smem, vmem, smem] + [vmem] * 7,
        out_specs=[vmem] * 9,
        out_shape=[
            jax.ShapeDtypeStruct((ROWS * hid, w_first.shape[0] * ROWS), bf16),
            tiles_like(hid, COLS),
            jax.ShapeDtypeStruct((hid, hid), bf16),
            tiles_like(hid, COLS),
            jax.ShapeDtypeStruct((bands, hid + 16), bf16),
            tiles_like(groups, ROWS, COLS),
            tiles_like(ROWS, ROWS, COLS),
            tiles_like(ROWS, ROWS, COLS),
            tiles_like(ROWS, COLS),
        ],
        scratch_shapes=[
            pltpu.VMEM((COLS, COLS), f32),
            pltpu.VMEM((COLS, pl.cdiv(bands, COLS) * COLS), f32),
        ],
        name="prepare",
    )(
        sun_index,
        block_slot.reshape(1, -1),
        albedo,
        sun_table,
        solar.reshape(1, -1),
        w_first,
        b_first.reshape(1, -1),
        w_second,
        b_second.reshape(1, -1),
        w_third,
        b_third.reshape(1, -1),
    )
    gas_rows = gases.transpose(1, 0, 2, 3).reshape(levels, gas * ROWS, COLS)
    cols, prepared, gas_rows = lax.optimization_barrier((cols, prepared, gas_rows))
    rows = exchange_rows(rows_one, rows_two, flags, cols)

    packed = packed_tiles(fields, levels)
    state, heating, one, two, rows_one, rows_two, face, side_face = pl.pallas_call(
        first_kernel,
        in_specs=[vmem] * 8 + [smem] + [vmem] * 10,
        out_specs=[vmem] * 8,
        out_shape=[
            tiles_like(ntr * levels * ROWS, COLS),
            tiles_like(levels, ROWS, COLS),
        ]
        + [tiles_like(packed_tiles(ntr, levels), ROWS, COLS)] * 2
        + [tiles_like(row_payload(ntr, levels), COLS)] * 2
        + [tiles_like(levels, 6, ROWS, COLS), tiles_like(4, ROWS, COLS)],
        scratch_shapes=[
            pltpu.VMEM((fields * levels * ROWS, COLS), f32),
            pltpu.VMEM((2 * packed, ROWS, COLS), f32),
            pltpu.VMEM((packed, ROWS, COLS), f32),
            pltpu.VMEM((packed, ROWS, COLS), f32),
            pltpu.VMEM((packed, ROWS, COLS), f32),
            pltpu.VMEM((levels, ntr * ROWS, COLS), bf16),
            pltpu.VMEM((ROWS * hid, 2 * COLS), bf16),
            pltpu.VMEM((ROWS * hid, 2 * COLS), bf16),
            pltpu.VMEM((ROWS * levels // 2 + 2, hid + 16, 2 * COLS), bf16),
            pltpu.VMEM((groups, ROWS, 2 * COLS), f32),
            pltpu.VMEM((groups, ROWS, 2 * COLS), f32),
            pltpu.VMEM((levels + 1, groups, ROWS, COLS), f32),
            pltpu.VMEM((levels + 1, groups, ROWS, COLS), f32),
            pltpu.VMEM((groups, ROWS, COLS), f32),
            pltpu.VMEM((ROWS, levels + 1, ROWS, COLS), f32),
        ],
        name="transport_radiation",
    )(tracers, winds, *own, *cols, *rows, flags, gas_rows, *prepared)

    own = (one, two)
    cols = swap_pairs(one, two, "lon", True)
    rows = exchange_rows(rows_one, rows_two, flags, cols)
    final = pl.pallas_call(
        last_kernel,
        in_specs=[vmem] * 9 + [smem],
        out_specs=vmem,
        out_shape=tiles_like(ntr, levels, ROWS, COLS),
        scratch_shapes=[
            pltpu.VMEM((ntr * levels * ROWS, COLS), f32),
            pltpu.VMEM((2 * packed_tiles(ntr, levels), ROWS, COLS), f32),
        ]
        + [pltpu.VMEM((packed_tiles(ntr, levels), ROWS, COLS), f32)] * 3,
        name="last_transport",
    )(state, face, side_face, *own, *cols, *rows, flags)
    return final, heating


def solution(mesh):
    grid = P(None, None, "lat", "lon")
    in_specs = (grid, grid, grid) + (P("lat", "lon"),) * 3 + (P(),) * 8
    out_specs = (grid, P(None, "lat", "lon"))
    return jax.shard_map(body, mesh=mesh, in_specs=in_specs, out_specs=out_specs, check_vma=False)
```

```python
import functools
import math

import jax
import jax.numpy as jnp
from jax import lax
from jax.experimental import pallas as pl
from jax.experimental.pallas import tpu as pltpu
from jax.sharding import PartitionSpec as P

tau_scale = 0.05
mu_floor = 0.05
heat_scale = 30.0
diffuse_factor = 1.66
log2e = 1.4426950408889634

ROWS = 8
COLS = 128
RIM = 2
SLOTS = COLS // RIM
HAS_AFTER, HAS_BEFORE, LAT_EVEN, LON_EVEN = range(4)


def lane_id():
    return lax.broadcasted_iota(jnp.int32, (ROWS, COLS), 1)


def row_id():
    return lax.broadcasted_iota(jnp.int32, (ROWS, COLS), 0)


def ahead_row(tile, beside):
    return pltpu.roll(jnp.where(row_id() == 0, beside, tile), ROWS - 1, 0)


def behind_row(tile, beside):
    return pltpu.roll(jnp.where(row_id() == ROWS - 1, beside, tile), 1, 0)


def flux(face, here, there):
    return jnp.maximum(face, 0.0) * here + jnp.minimum(face, 0.0) * there


def next_col(tile, rim):
    return jnp.where(lane_id() == COLS - 1, rim, pltpu.roll(tile, COLS - 1, 1))


def col_change(face, first, tile, rim):
    out = flux(face, tile, next_col(tile, rim))
    return out - jnp.where(lane_id() == 0, flux(first, rim, tile), pltpu.roll(out, 1, 1))


def col_faces(wind, rim):
    return 0.5 * (wind + next_col(wind, rim)), 0.5 * (rim + wind)


def row_faces(main, rows):
    return 0.5 * (main + ahead_row(main, rows)), 0.5 * (rows + ahead_row(rows, main))


def row_changes(face, main, rows):
    out = flux(face[0], main, ahead_row(main, rows))
    rim = flux(face[1], rows, ahead_row(rows, main))
    return out - behind_row(out, rim), rim - behind_row(rim, out)


def two_steps(main, rows, side, corner, next_side, face, inside):
    north, south = row_changes(face[4:], main, rows)
    main1 = main - col_change(face[0], face[1], main, side) - north
    rows1 = rows - col_change(face[2], face[3], rows, corner) - south
    rows1 = jnp.where(inside > 0.0, rows1, 0.0)
    north, _ = row_changes(face[4:], main1, rows1)
    return main1 - col_change(face[0], face[1], main1, next_side) - north


def pack_sides(tile, slot, packs):
    head, tail = packs
    own = lane_id() // RIM
    moved = pltpu.roll(tile, RIM * slot, 1)
    head = jnp.where(own == slot, moved, head)
    tail = jnp.where(own == lax.rem(slot + SLOTS - 1, SLOTS), moved, tail)
    return head, tail


def tile_at(tile):
    return pl.ds(pl.multiple_of(tile * ROWS, ROWS), ROWS)


def kept_rows(flags):
    after = (row_id() == 0) & (flags[HAS_AFTER] > 0)
    before = (row_id() == ROWS - 1) & (flags[HAS_BEFORE] > 0)
    return jnp.where(after | before, 1.0, 0.0)


def each_level(levels, step, carry, block):
    def trip(at, carry):
        for k in range(block):
            carry = step(block * at + k, carry)
        return carry

    return lax.fori_loop(0, levels // block, trip, carry)


def place(field, level, levels):
    per = SLOTS // levels
    return field // per, (field % per) * levels + level


def packed_tiles(fields, levels):
    return pl.cdiv(fields * levels, SLOTS)


def pack_fields(sources, levels, even, one_ref, two_ref):
    count = packed_tiles(len(sources), levels)
    zero = jnp.zeros((ROWS, COLS), jnp.float32)

    def step(level, packs):
        packs = list(packs)
        for field, source in enumerate(sources):
            tile, slot = place(field, level, levels)
            packs[tile] = pack_sides(source(level), slot, packs[tile])
        return tuple(packs)

    packs = each_level(levels, step, ((zero, zero),) * count, 8)
    for tile, (head, tail) in enumerate(packs):
        tail = pltpu.roll(tail, RIM, 1)
        one_ref[tile] = jnp.where(even, tail, head)
        two_ref[tile] = jnp.where(even, head, tail)


def pack_rows(sources, even, one, two):
    at = 0
    total = sum(ref.shape[0] for ref in sources) // ROWS
    for ref in sources:
        tiles = ref.shape[0] // ROWS
        for row in range(RIM):
            head = ref[pl.ds(row, tiles, stride=ROWS), :]
            tail = ref[pl.ds(ROWS - RIM + row, tiles, stride=ROWS), :]
            one[pl.ds(row * total + at, tiles), :] = jnp.where(even, tail, head)
            two[pl.ds(row * total + at, tiles), :] = jnp.where(even, head, tail)
        at += tiles


def corner_rows(packed):
    return pl.cdiv(2 * RIM * packed, ROWS) * ROWS


def row_payload(fields, levels):
    return RIM * fields * levels + corner_rows(packed_tiles(fields, levels))


def pack_kernel(levels, flags, tracers, winds, one, two, one_rows, two_rows):
    sources = []
    for ref in (tracers, winds):
        for f in range(ref.shape[0] // (levels * ROWS)):
            base = f * levels * ROWS
            sources.append(
                lambda level, ref=ref, base=base: ref[
                    pl.ds(pl.multiple_of(base + level * ROWS, ROWS), ROWS), :
                ]
            )
    pack_rows((tracers, winds), flags[LAT_EVEN] > 0, one_rows, two_rows)
    pack_fields(sources, levels, flags[LON_EVEN] > 0, one, two)


def in_order(even, one, two):
    return jnp.where(even, one, two), jnp.where(even, two, one)


def corner_kernel(one_in, two_in, flags, cols_one, cols_two, one, two):
    del one_in, two_in
    lon_even, lat_even = flags[LON_EVEN] > 0, flags[LAT_EVEN] > 0
    count = cols_one.shape[0]
    base = one.shape[0] - corner_rows(count)
    for tile in range(count):
        for side, block in enumerate(in_order(lon_even, cols_one[tile], cols_two[tile])):
            at = base + RIM * (side * count + tile)
            head, tail = block[0:RIM], block[ROWS - RIM : ROWS]
            one[at : at + RIM, :] = jnp.where(lat_even, tail, head)
            two[at : at + RIM, :] = jnp.where(lat_even, head, tail)
    for at in range(base + 2 * RIM * count, one.shape[0], RIM):
        one[at : at + RIM, :] = jnp.zeros((RIM, COLS), jnp.float32)
        two[at : at + RIM, :] = jnp.zeros((RIM, COLS), jnp.float32)


def unpack_rows(even, rows_one, rows_two, rim_ref, corner_ref, tiles, packed):
    for row in range(RIM):
        here = pl.ds(row * tiles, tiles)
        after, before = in_order(even, rows_one[here, :], rows_two[here, :])
        rim_ref[pl.ds(row, tiles, stride=ROWS), :] = after
        rim_ref[pl.ds(ROWS - RIM + row, tiles, stride=ROWS), :] = before
    for tile in range(2 * packed):
        at = RIM * (tiles + tile)
        after, before = in_order(even, rows_one[at : at + RIM, :], rows_two[at : at + RIM, :])
        corner_ref[tile, 0:RIM, :] = after
        corner_ref[tile, ROWS - RIM : ROWS, :] = before


def paired(after, before):
    return jnp.where(lane_id() % 2 == 0, after, before)


def side_tiles(even, own_one, own_two, cols_one, cols_two, corner_ref, tile, packed):
    right, left = in_order(even, cols_one[tile], cols_two[tile])
    tail, head = in_order(even, own_one[tile], own_two[tile])
    return (
        paired(right, left),
        paired(pltpu.roll(right, COLS - 1, 1), pltpu.roll(head, 1, 1)),
        paired(pltpu.roll(tail, COLS - 1, 1), pltpu.roll(left, 1, 1)),
        paired(corner_ref[tile], corner_ref[packed + tile]),
    )


def side_faces(tiles):
    low = lane_id() < COLS // 2
    half = [pltpu.roll(t, COLS // 2, 1) for t in tiles]
    u, after, before, _ = [jnp.where(low, t, h) for t, h in zip(tiles, half)]
    v, _, _, corner = [jnp.where(low, h, t) for t, h in zip(tiles, half)]
    return (0.5 * (u + after), 0.5 * (before + u), *row_faces(v, corner))


def side_step(tiles, face):
    here, after, before, corner = tiles
    east = flux(face[0], here, after) - flux(face[1], before, here)
    return here - east - row_changes(face[2:], here, corner)[0]


def from_side(ref, field, level, levels):
    tile, slot = place(field, level, levels)
    return pltpu.roll(ref[tile], COLS - 1 - RIM * slot, 1)


def first_kernel(
    tracers,
    winds,
    own_one,
    own_two,
    cols_one,
    cols_two,
    rows_one,
    rows_two,
    flags,
    gases,
    w1,
    b1,
    w2,
    b2,
    w3,
    lsolar,
    kappa,
    lground,
    scaled,
    state,
    heating,
    next_one,
    next_two,
    next_rows_one,
    next_rows_two,
    face,
    side_face,
    rim_ref,
    corner_ref,
    side_ref,
    next_side_ref,
    side_rim_ref,
    xs,
    hid_a,
    hid_b,
    hidden,
    logits_a,
    logits_b,
    depth_a,
    depth_b,
    weight,
    sums,
):
    depths = (depth_a, depth_b)
    ntr, levels = tracers.shape[0], tracers.shape[1]
    fields = ntr + winds.shape[0]
    packed = packed_tiles(fields, levels)
    groups = lsolar.shape[0]
    hid = b1.shape[0]
    lon_even, lat_even = flags[LON_EVEN] > 0, flags[LAT_EVEN] > 0
    unpack_rows(lat_even, rows_one, rows_two, rim_ref, corner_ref, fields * levels, packed)
    keep = kept_rows(flags)
    sides = [
        side_tiles(lon_even, own_one, own_two, cols_one, cols_two, corner_ref, tile, packed)
        for tile in range(packed)
    ]
    of_sides = side_faces(sides[packed - 1])
    for k, tile in enumerate(of_sides):
        side_face[k] = tile
    for tile in range(packed):
        side_ref[tile] = sides[tile][0]
        side_rim_ref[tile] = sides[tile][3]
        if tile < packed - 1:
            next_side_ref[tile] = side_step(sides[tile], of_sides)

    def transport(level, carry):
        def rows_of(field):
            return rim_ref[tile_at(field * levels + level), :]

        tiles = (
            *col_faces(winds[0, level], from_side(side_ref, ntr, level, levels)),
            *col_faces(rows_of(ntr), from_side(side_rim_ref, ntr, level, levels)),
            *row_faces(winds[1, level], rows_of(ntr + 1)),
        )
        for k, tile in enumerate(tiles):
            face[level, k] = tile
        out = []
        for f in range(ntr):
            q = two_steps(
                tracers[f, level],
                rows_of(f),
                from_side(side_ref, f, level, levels),
                from_side(side_rim_ref, f, level, levels),
                from_side(next_side_ref, f, level, levels),
                tiles,
                keep,
            )
            state[tile_at(f * levels + level), :] = q
            out.append(q)
        xs[level] = jnp.concatenate(out, 0).astype(jnp.bfloat16)
        return carry

    each_level(levels, transport, 0, 4)

    diffuse = diffuse_factor * tau_scale
    pairs = levels // 2
    depths[0][0] = jnp.zeros((groups, ROWS, COLS), jnp.float32)
    depths[1][0] = jnp.zeros((groups, ROWS, COLS), jnp.float32)
    ones = jnp.ones((w3.shape[1] - hid, 2 * COLS), jnp.bfloat16)

    def silu(half):
        return (half + half * jnp.tanh(half)).astype(jnp.bfloat16)

    def layer_one(pair, out):
        x = jnp.concatenate(
            [jnp.concatenate([gases[2 * pair + k], xs[2 * pair + k]], 0) for k in range(2)], 1
        )
        wide = jnp.concatenate([b1[...]] * 2, 1)
        part = ROWS // 2
        for at in range(0, ROWS, part):
            mine = w1[at * hid : (at + part) * hid, :]
            y = jnp.dot(mine, x, preferred_element_type=jnp.float32)
            for k in range(part):
                out[(at + k) * hid : (at + k + 1) * hid, :] = silu(
                    y[k * hid : (k + 1) * hid] + wide
                )

    def layer_two(pair, source, at=lambda row, pair: row * pairs + pair):
        wide = jnp.concatenate([b2[...]] * 2, 1)
        for row in range(ROWS):
            y = source[row * hid : (row + 1) * hid, :]
            y = silu(jnp.dot(w2[...], y, preferred_element_type=jnp.float32) + wide)
            hidden[at(row, pair)] = jnp.concatenate([y, ones], 0)

    def layers(step, carry):
        layer_one(2 * step, hid_a)

        layer_two(
            2 * step - 1,
            hid_b,
            lambda row, pair: jnp.where(step == 0, ROWS * pairs, row * pairs + pair),
        )

        layer_one(2 * step + 1, hid_b)
        layer_two(2 * step, hid_a)
        return carry

    lax.fori_loop(0, pairs // 2, layers, 0)
    layer_two(pairs - 1, hid_b)

    def third(at, buf):
        buf[...] = jnp.dot(w3[...], hidden[at], preferred_element_type=jnp.float32).reshape(
            groups, ROWS, 2 * COLS
        )

    def optical(pair, depth, buf):
        t = buf[...] * log2e
        soft = jnp.maximum(t, jnp.log2(1.0 + jnp.exp2(jnp.minimum(t, 126.0))))
        d = depth[2 * pair] + soft[:, :, :COLS]
        depth[2 * pair + 1] = d
        depth[2 * pair + 2] = d + soft[:, :, COLS:]

    def light(row, level, depth):
        d = depth[level]
        direct = jnp.exp2(lsolar[...] - d * kappa[row][None])
        upward = jnp.exp2(weight[...] + d * diffuse)
        sums[row, level] = jnp.sum(direct - upward, 0)

    def close(row, depth):
        total = depth[levels]
        weight[...] = (
            lsolar[...] + lground[row][None] - total * (kappa[row] + diffuse)[None]
        )
        light(row, levels, depth)

    def both(row, depth, before):
        close(row - 1, before)

        def step(trip, carry):
            for k, buf in enumerate(bufs):
                pair = 2 * trip + k
                optical(pair, depth, buf)
                light(row - 1, 2 * pair, before)
                light(row - 1, 2 * pair + 1, before)
                third(row * pairs + pair + 2, buf)
            return carry

        lax.fori_loop(0, pairs // 2, step, 0)

    def only_optical(trip, carry):
        for k, buf in enumerate(bufs):
            optical(2 * trip + k, depths[0], buf)
            third(2 * trip + k + 2, buf)
        return carry

    bufs = (logits_a, logits_b)
    third(0, logits_a)
    third(1, logits_b)
    lax.fori_loop(0, pairs // 2, only_optical, 0)

    def two_rows(step, carry):
        both(2 * step + 1, depths[1], depths[0])
        both(2 * step + 2, depths[0], depths[1])
        return carry

    lax.fori_loop(0, ROWS // 2 - 1, two_rows, 0)
    both(ROWS - 1, depths[1], depths[0])
    close(ROWS - 1, depths[1])

    def only_light(pair, carry):
        light(ROWS - 1, 2 * pair, depths[1])
        light(ROWS - 1, 2 * pair + 1, depths[1])
        return carry

    lax.fori_loop(0, pairs, only_light, 0)

    for row in range(ROWS):
        change = sums[row, 0:levels] - sums[row, 1 : levels + 1]
        heating[:, row, :] = jnp.sum(change, 1) * scaled[row : row + 1, :]

    def add(level, carry):
        tile = tile_at(level)
        state[tile, :] = state[tile, :] + heating[level]
        return carry

    each_level(levels, add, 0, 8)
    pack_rows((state,), lat_even, next_rows_one, next_rows_two)
    pack_fields(
        [lambda level, f=f: state[tile_at(f * levels + level), :] for f in range(ntr)],
        levels,
        lon_even,
        next_one,
        next_two,
    )


def last_kernel(
    tracers,
    face,
    side_face,
    own_one,
    own_two,
    cols_one,
    cols_two,
    rows_one,
    rows_two,
    flags,
    out,
    rim_ref,
    corner_ref,
    side_ref,
    next_side_ref,
    side_rim_ref,
):
    ntr, levels = out.shape[0], out.shape[1]
    packed = packed_tiles(ntr, levels)
    lon_even, lat_even = flags[LON_EVEN] > 0, flags[LAT_EVEN] > 0
    unpack_rows(lat_even, rows_one, rows_two, rim_ref, corner_ref, ntr * levels, packed)
    keep = kept_rows(flags)
    of_sides = [side_face[k] for k in range(4)]
    for tile in range(packed):
        sides = side_tiles(
            lon_even, own_one, own_two, cols_one, cols_two, corner_ref, tile, packed
        )
        side_ref[tile] = sides[0]
        side_rim_ref[tile] = sides[3]
        next_side_ref[tile] = side_step(sides, of_sides)

    def transport(level, carry):
        tiles = [face[level, k] for k in range(6)]
        for f in range(ntr):
            out[f, level] = two_steps(
                tracers[tile_at(f * levels + level), :],
                rim_ref[tile_at(f * levels + level), :],
                from_side(side_ref, f, level, levels),
                from_side(side_rim_ref, f, level, levels),
                from_side(next_side_ref, f, level, levels),
                tiles,
                keep,
            )
        return carry

    each_level(levels, transport, 0, 4)


def prepare_kernel(
    index,
    slot,
    ground,
    table,
    solar,
    w_first,
    b_first,
    w_second,
    b_second,
    w_third,
    b_third,
    w1,
    b1,
    w2,
    b2,
    w3,
    lsolar,
    kappa,
    lground,
    scaled,
    square,
    wide,
):
    feat, hid = w_first.shape
    bands = solar.shape[1]

    def column(ref, factor):
        square[:, 0 : ref.shape[1]] = jnp.broadcast_to(ref[...], (COLS, ref.shape[1])) * factor
        return jnp.transpose(square[...])[0 : ref.shape[1]]

    square[...] = jnp.zeros(square.shape, jnp.float32)
    b1[...] = column(b_first, 0.5)
    b2[...] = column(b_second, 0.5)

    square[...] = jnp.zeros(square.shape, jnp.float32)
    square[0:hid, 0:hid] = w_second[...].astype(jnp.float32) * 0.5
    w2[...] = jnp.transpose(square[...])[0:hid, 0:hid].astype(jnp.bfloat16)

    square[...] = jnp.zeros(square.shape, jnp.float32)
    square[0:feat, 0:hid] = w_first[...].astype(jnp.float32) * 0.5
    by_unit = jnp.transpose(square[...])[0:hid].astype(jnp.bfloat16)
    source = lax.broadcasted_iota(jnp.int32, (COLS, COLS), 0)
    lane = lax.broadcasted_iota(jnp.int32, (COLS, COLS), 1)
    spread = jnp.where(lane // ROWS == source, 1.0, 0.0).astype(jnp.bfloat16)
    by_lane = jnp.dot(by_unit, spread, preferred_element_type=jnp.float32)
    of_row = lax.broadcasted_iota(jnp.int32, (hid, COLS), 1) % ROWS
    for row in range(ROWS):
        w1[row * hid : (row + 1) * hid, :] = jnp.where(of_row == row, by_lane, 0.0).astype(
            jnp.bfloat16
        )

    wide[...] = jnp.zeros(wide.shape, jnp.float32)
    wide[0:hid, 0:bands] = w_third[...].astype(jnp.float32)
    rest = b_third[...]
    for k in range(3):
        part = rest.astype(jnp.bfloat16).astype(jnp.float32)
        wide[hid + k : hid + k + 1, 0:bands] = part
        rest = rest - part
    w3[...] = jnp.transpose(wide[...])[0:bands, 0 : w3.shape[1]].astype(jnp.bfloat16)

    wide[:, 0:bands] = jnp.broadcast_to(jnp.log2(solar[...]), (COLS, bands))
    lsolar[...] = jnp.transpose(wide[...])[0:bands].reshape(lsolar.shape)

    ids = index[...]
    cosine = jnp.zeros((ROWS, COLS), jnp.float32)
    for entry in range(1, table.shape[0]):
        cosine = jnp.where(ids == entry, table[entry], cosine)
    slant = tau_scale / jnp.maximum(cosine, mu_floor)
    lg = jnp.log2(ground[...].astype(jnp.float32))
    for row in range(ROWS):
        kappa[row] = jnp.broadcast_to(slant[row : row + 1], (ROWS, COLS))
        lground[row] = jnp.broadcast_to(lg[row : row + 1], (ROWS, COLS))
        lit = jnp.where(slot[0, row] >= 0, heat_scale, 0.0)
        scaled[row : row + 1, :] = lit * cosine[row : row + 1]


vmem = pl.BlockSpec(memory_space=pltpu.VMEM)
smem = pl.BlockSpec(memory_space=pltpu.SMEM)
f32 = jnp.float32


def tiles_like(*shape):
    return jax.ShapeDtypeStruct(shape, f32)


def held(*shape, dtype=f32):
    return pltpu.VMEM(shape, dtype)


def near(*arrays):
    return [pltpu.with_memory_space_constraint(x, pltpu.VMEM) for x in arrays]


def swap_pairs(one, two, axis, ring):
    count = lax.axis_size(axis)
    near = [(i, i ^ 1) for i in range(count)]
    far = [(i, (i - 1 if i % 2 == 0 else i + 1) % count) for i in range(count)]
    if not ring:
        far = [(i, j) for i, j in far if abs(i - j) == 1]
    return lax.ppermute(one, axis, near), lax.ppermute(two, axis, far)


def add_corners(one, two, flags, cols):
    return pl.pallas_call(
        corner_kernel,
        in_specs=[vmem] * 2 + [smem] + [vmem] * 2,
        out_specs=[vmem] * 2,
        out_shape=[held(*one.shape)] * 2,
        input_output_aliases={0: 0, 1: 1},
        name="add_corners",
    )(*near(one, two), flags, *near(*cols))


def body(
    tracers,
    winds,
    gases,
    sun_index,
    block_slot,
    albedo,
    sun_table,
    solar,
    w_first,
    b_first,
    w_second,
    b_second,
    w_third,
    b_third,
):
    ntr, levels, clat, width = tracers.shape
    fields = ntr + winds.shape[0]
    gas = gases.shape[0]
    hid = w_first.shape[1]
    bands = solar.shape[0]
    if lax.axis_size("lat") % 2 or lax.axis_size("lon") % 2:
        raise ValueError("unsupported mesh")
    if (clat, width) != (ROWS, COLS) or w_first.shape[0] * ROWS != COLS or levels % 8 or 2 * levels != SLOTS or ntr % 2 or SLOTS % levels or bands % ROWS:
        raise ValueError("unsupported sizes")

    flat = (tracers.reshape(-1, COLS), winds.reshape(-1, COLS))
    columns = held(packed_tiles(fields, levels), ROWS, COLS)
    lat, lats = lax.axis_index("lat"), lax.axis_size("lat")
    flags = [lat < lats - 1, lat > 0, lat % 2 == 0, lax.axis_index("lon") % 2 == 0]
    flags = jnp.stack(flags).astype(jnp.int32)
    one, two, rows_one, rows_two = pl.pallas_call(
        functools.partial(pack_kernel, levels),
        in_specs=[smem] + [vmem] * 2,
        out_specs=[vmem] * 4,
        out_shape=[columns] * 2 + [held(row_payload(fields, levels), COLS)] * 2,
        name="pack",
    )(flags, *flat)
    own = (one, two)
    cols = swap_pairs(one, two, "lon", True)

    rows = add_corners(rows_one, rows_two, flags, cols)
    rows, gases, sun_index = lax.optimization_barrier((rows, gases, sun_index))

    groups = bands // ROWS
    bf16 = jnp.bfloat16
    prepared = pl.pallas_call(
        prepare_kernel,
        in_specs=[vmem, smem, vmem, smem] + [vmem] * 7,
        out_specs=[vmem] * 9,
        out_shape=[
            held(ROWS * hid, w_first.shape[0] * ROWS, dtype=bf16),
            held(hid, COLS),
            held(hid, hid, dtype=bf16),
            held(hid, COLS),
            held(bands, hid + 16, dtype=bf16),
            held(groups, ROWS, COLS),
            held(ROWS, ROWS, COLS),
            held(ROWS, ROWS, COLS),
            held(ROWS, COLS),
        ],
        scratch_shapes=[
            pltpu.VMEM((COLS, COLS), f32),
            pltpu.VMEM((COLS, pl.cdiv(bands, COLS) * COLS), f32),
        ],
        name="prepare",
    )(
        sun_index,
        block_slot.reshape(1, -1),
        albedo,
        sun_table,
        solar.reshape(1, -1),
        w_first,
        b_first.reshape(1, -1),
        w_second,
        b_second.reshape(1, -1),
        w_third,
        b_third.reshape(1, -1),
    )
    gas_rows = gases.transpose(1, 0, 2, 3).reshape(levels, gas * ROWS, COLS)
    rows = swap_pairs(*rows, "lat", False)

    packed = packed_tiles(fields, levels)
    state, heating, one, two, rows_one, rows_two, face, side_face = pl.pallas_call(
        first_kernel,
        in_specs=[vmem] * 8 + [smem] + [vmem] * 10,
        out_specs=[vmem] * 8,
        out_shape=[held(ntr * levels * ROWS, COLS), tiles_like(levels, ROWS, COLS)]
        + [held(packed_tiles(ntr, levels), ROWS, COLS)] * 2
        + [held(row_payload(ntr, levels), COLS)] * 2
        + [held(levels, 6, ROWS, COLS), held(4, ROWS, COLS)],
        scratch_shapes=[
            pltpu.VMEM((fields * levels * ROWS, COLS), f32),
            pltpu.VMEM((2 * packed, ROWS, COLS), f32),
            pltpu.VMEM((packed, ROWS, COLS), f32),
            pltpu.VMEM((packed, ROWS, COLS), f32),
            pltpu.VMEM((packed, ROWS, COLS), f32),
            pltpu.VMEM((levels, ntr * ROWS, COLS), bf16),
            pltpu.VMEM((ROWS * hid, 2 * COLS), bf16),
            pltpu.VMEM((ROWS * hid, 2 * COLS), bf16),
            pltpu.VMEM((ROWS * levels // 2 + 2, hid + 16, 2 * COLS), bf16),
            pltpu.VMEM((groups, ROWS, 2 * COLS), f32),
            pltpu.VMEM((groups, ROWS, 2 * COLS), f32),
            pltpu.VMEM((levels + 1, groups, ROWS, COLS), f32),
            pltpu.VMEM((levels + 1, groups, ROWS, COLS), f32),
            pltpu.VMEM((groups, ROWS, COLS), f32),
            pltpu.VMEM((ROWS, levels + 1, ROWS, COLS), f32),
        ],
        compiler_params=pltpu.CompilerParams(vmem_limit_bytes=28 << 20),
        name="transport_radiation",
    )(*near(tracers, winds, *own, *cols, *rows), flags, *near(gas_rows, *prepared))

    own = (one, two)
    cols = swap_pairs(one, two, "lon", True)
    rows = swap_pairs(*add_corners(rows_one, rows_two, flags, cols), "lat", False)
    final = pl.pallas_call(
        last_kernel,
        in_specs=[vmem] * 9 + [smem],
        out_specs=vmem,
        out_shape=tiles_like(ntr, levels, ROWS, COLS),
        scratch_shapes=[
            pltpu.VMEM((ntr * levels * ROWS, COLS), f32),
            pltpu.VMEM((2 * packed_tiles(ntr, levels), ROWS, COLS), f32),
        ]
        + [pltpu.VMEM((packed_tiles(ntr, levels), ROWS, COLS), f32)] * 3,
        compiler_params=pltpu.CompilerParams(vmem_limit_bytes=8 << 20),
        name="last_transport",
    )(*near(state, face, side_face, *own, *cols, *rows), flags)
    return final, heating


def solution(mesh):
    grid = P(None, None, "lat", "lon")
    in_specs = (grid, grid, grid) + (P("lat", "lon"),) * 3 + (P(),) * 8
    out_specs = (grid, P(None, "lat", "lon"))
    return jax.shard_map(body, mesh=mesh, in_specs=in_specs, out_specs=out_specs, check_vma=False)
```

```python
import functools
import math

import jax
import jax.numpy as jnp
from jax import lax
from jax.experimental import pallas as pl
from jax.experimental.pallas import tpu as pltpu
from jax.sharding import PartitionSpec as P

tau_scale = 0.05
mu_floor = 0.05
heat_scale = 30.0
diffuse_factor = 1.66
log2e = 1.4426950408889634

ROWS = 8
COLS = 128
RIM = 2
SLOTS = COLS // RIM
HAS_AFTER, HAS_BEFORE, LAT_EVEN, LON_EVEN = range(4)


def choose(flag, one, two):
    return jnp.where(jnp.broadcast_to(flag, one.shape) > 0.0, one, two)


def lane_id():
    return lax.broadcasted_iota(jnp.int32, (ROWS, COLS), 1)


def row_id():
    return lax.broadcasted_iota(jnp.int32, (ROWS, COLS), 0)


def ahead_row(tile, beside):
    return pltpu.roll(jnp.where(row_id() == 0, beside, tile), ROWS - 1, 0)


def behind_row(tile, beside):
    return pltpu.roll(jnp.where(row_id() == ROWS - 1, beside, tile), 1, 0)


def flux(face, here, there):
    return jnp.maximum(face, 0.0) * here + jnp.minimum(face, 0.0) * there


def next_col(tile, rim):
    return jnp.where(lane_id() == COLS - 1, rim, pltpu.roll(tile, COLS - 1, 1))


def col_change(face, first, tile, rim):
    out = flux(face, tile, next_col(tile, rim))
    return out - jnp.where(lane_id() == 0, flux(first, rim, tile), pltpu.roll(out, 1, 1))


def col_faces(wind, rim):
    return 0.5 * (wind + next_col(wind, rim)), 0.5 * (rim + wind)


def row_faces(main, rows):
    return 0.5 * (main + ahead_row(main, rows)), 0.5 * (rows + ahead_row(rows, main))


def row_changes(face, main, rows):
    out = flux(face[0], main, ahead_row(main, rows))
    rim = flux(face[1], rows, ahead_row(rows, main))
    return out - behind_row(out, rim), rim - behind_row(rim, out)


def two_steps(main, rows, side, corner, next_side, face, inside):
    north, south = row_changes(face[4:], main, rows)
    main1 = main - col_change(face[0], face[1], main, side) - north
    rows1 = rows - col_change(face[2], face[3], rows, corner) - south
    rows1 = jnp.where(inside > 0.0, rows1, 0.0)
    north, _ = row_changes(face[4:], main1, rows1)
    return main1 - col_change(face[0], face[1], main1, next_side) - north


def pack_sides(tile, slot, packs):
    head, tail = packs
    own = lane_id() // RIM
    moved = pltpu.roll(tile, RIM * slot, 1)
    head = jnp.where(own == slot, moved, head)
    tail = jnp.where(own == lax.rem(slot + SLOTS - 1, SLOTS), moved, tail)
    return head, tail


def tile_at(tile):
    return pl.ds(pl.multiple_of(tile * ROWS, ROWS), ROWS)


def kept_rows(flags):
    after = (row_id() == 0) & (flags[HAS_AFTER] > 0.0)
    before = (row_id() == ROWS - 1) & (flags[HAS_BEFORE] > 0.0)
    return jnp.where(after | before, 1.0, 0.0)


def each_level(levels, step, carry, block):
    def trip(at, carry):
        for k in range(block):
            carry = step(block * at + k, carry)
        return carry

    return lax.fori_loop(0, levels // block, trip, carry)


def place(field, level, levels):
    per = SLOTS // levels
    return field // per, (field % per) * levels + level


def packed_tiles(fields, levels):
    return pl.cdiv(fields * levels, SLOTS)


def pack_fields(sources, levels, even, one_ref, two_ref):
    count = packed_tiles(len(sources), levels)
    zero = jnp.zeros((ROWS, COLS), jnp.float32)

    def step(level, packs):
        packs = list(packs)
        for field, source in enumerate(sources):
            tile, slot = place(field, level, levels)
            packs[tile] = pack_sides(source(level), slot, packs[tile])
        return tuple(packs)

    packs = each_level(levels, step, ((zero, zero),) * count, 8)
    for tile, (head, tail) in enumerate(packs):
        tail = pltpu.roll(tail, RIM, 1)
        one_ref[tile] = choose(even, tail, head)
        two_ref[tile] = choose(even, head, tail)


def pack_rows(sources, even, one, two):
    at = 0
    total = sum(ref.shape[0] for ref in sources) // ROWS
    for ref in sources:
        tiles = ref.shape[0] // ROWS
        for row in range(RIM):
            head = ref[pl.ds(row, tiles, stride=ROWS), :]
            tail = ref[pl.ds(ROWS - RIM + row, tiles, stride=ROWS), :]
            one[pl.ds(row * total + at, tiles), :] = choose(even, tail, head)
            two[pl.ds(row * total + at, tiles), :] = choose(even, head, tail)
        at += tiles


def corner_rows(packed):
    return pl.cdiv(2 * RIM * packed, ROWS) * ROWS


def row_payload(fields, levels):
    return RIM * fields * levels + corner_rows(packed_tiles(fields, levels))


def pack_kernel(levels, flags, tracers, winds, one, two, one_rows, two_rows):
    sources = []
    for ref in (tracers, winds):
        for f in range(ref.shape[0] // (levels * ROWS)):
            base = f * levels * ROWS
            sources.append(
                lambda level, ref=ref, base=base: ref[
                    pl.ds(pl.multiple_of(base + level * ROWS, ROWS), ROWS), :
                ]
            )
    pack_rows((tracers, winds), flags[LAT_EVEN, 0:1], one_rows, two_rows)
    pack_fields(sources, levels, flags[LON_EVEN, 0:1], one, two)


def in_order(even, one, two):
    return choose(even, one, two), choose(even, two, one)


def corner_kernel(one_in, two_in, flags, cols_one, cols_two, one, two):
    del one_in, two_in
    lon_even, lat_even = flags[LON_EVEN, 0:1], flags[LAT_EVEN, 0:1]
    count = cols_one.shape[0]
    base = one.shape[0] - corner_rows(count)
    for tile in range(count):
        for side, block in enumerate(in_order(lon_even, cols_one[tile], cols_two[tile])):
            at = base + RIM * (side * count + tile)
            head, tail = block[0:RIM], block[ROWS - RIM : ROWS]
            one[at : at + RIM, :] = choose(lat_even, tail, head)
            two[at : at + RIM, :] = choose(lat_even, head, tail)
    for at in range(base + 2 * RIM * count, one.shape[0], RIM):
        one[at : at + RIM, :] = jnp.zeros((RIM, COLS), jnp.float32)
        two[at : at + RIM, :] = jnp.zeros((RIM, COLS), jnp.float32)


def unpack_rows(even, rows_one, rows_two, rim_ref, corner_ref, tiles, packed):
    for row in range(RIM):
        here = pl.ds(row * tiles, tiles)
        after, before = in_order(even, rows_one[here, :], rows_two[here, :])
        rim_ref[pl.ds(row, tiles, stride=ROWS), :] = after
        rim_ref[pl.ds(ROWS - RIM + row, tiles, stride=ROWS), :] = before
    for tile in range(2 * packed):
        at = RIM * (tiles + tile)
        after, before = in_order(even, rows_one[at : at + RIM, :], rows_two[at : at + RIM, :])
        corner_ref[tile, 0:RIM, :] = after
        corner_ref[tile, ROWS - RIM : ROWS, :] = before


def paired(after, before):
    return jnp.where(lane_id() % 2 == 0, after, before)


def side_tiles(even, own_one, own_two, cols_one, cols_two, corner_ref, tile, packed):
    right, left = in_order(even, cols_one[tile], cols_two[tile])
    tail, head = in_order(even, own_one[tile], own_two[tile])
    return (
        paired(right, left),
        paired(pltpu.roll(right, COLS - 1, 1), pltpu.roll(head, 1, 1)),
        paired(pltpu.roll(tail, COLS - 1, 1), pltpu.roll(left, 1, 1)),
        paired(corner_ref[tile], corner_ref[packed + tile]),
    )


def side_faces(tiles):
    low = lane_id() < COLS // 2
    half = [pltpu.roll(t, COLS // 2, 1) for t in tiles]
    u, after, before, _ = [jnp.where(low, t, h) for t, h in zip(tiles, half)]
    v, _, _, corner = [jnp.where(low, h, t) for t, h in zip(tiles, half)]
    return (0.5 * (u + after), 0.5 * (before + u), *row_faces(v, corner))


def side_step(tiles, face):
    here, after, before, corner = tiles
    east = flux(face[0], here, after) - flux(face[1], before, here)
    return here - east - row_changes(face[2:], here, corner)[0]


def from_side(ref, field, level, levels):
    tile, slot = place(field, level, levels)
    return pltpu.roll(ref[tile], COLS - 1 - RIM * slot, 1)


def first_kernel(
    tracers,
    winds,
    own_one,
    own_two,
    cols_one,
    cols_two,
    rows_one,
    rows_two,
    flags,
    gases,
    w1,
    b1,
    w2,
    b2,
    w3,
    lsolar,
    kappa,
    lground,
    scaled,
    state,
    heating,
    next_one,
    next_two,
    next_rows_one,
    next_rows_two,
    face,
    side_face,
    rim_ref,
    corner_ref,
    side_ref,
    next_side_ref,
    side_rim_ref,
    xs,
    hid_a,
    hid_b,
    hidden,
    logits_a,
    logits_b,
    depth_a,
    depth_b,
    weight,
    sums,
):
    depths = (depth_a, depth_b)
    ntr, levels = tracers.shape[0], tracers.shape[1]
    fields = ntr + winds.shape[0]
    packed = packed_tiles(fields, levels)
    groups = lsolar.shape[0]
    hid = b1.shape[0]
    lon_even, lat_even = flags[LON_EVEN, 0:1], flags[LAT_EVEN, 0:1]
    unpack_rows(lat_even, rows_one, rows_two, rim_ref, corner_ref, fields * levels, packed)
    keep = kept_rows(flags)
    sides = [
        side_tiles(lon_even, own_one, own_two, cols_one, cols_two, corner_ref, tile, packed)
        for tile in range(packed)
    ]
    of_sides = side_faces(sides[packed - 1])
    for k, tile in enumerate(of_sides):
        side_face[k] = tile
    for tile in range(packed):
        side_ref[tile] = sides[tile][0]
        side_rim_ref[tile] = sides[tile][3]
        if tile < packed - 1:
            next_side_ref[tile] = side_step(sides[tile], of_sides)

    def transport(level, carry):
        def rows_of(field):
            return rim_ref[tile_at(field * levels + level), :]

        tiles = (
            *col_faces(winds[0, level], from_side(side_ref, ntr, level, levels)),
            *col_faces(rows_of(ntr), from_side(side_rim_ref, ntr, level, levels)),
            *row_faces(winds[1, level], rows_of(ntr + 1)),
        )
        for k, tile in enumerate(tiles):
            face[level, k] = tile
        out = []
        for f in range(ntr):
            q = two_steps(
                tracers[f, level],
                rows_of(f),
                from_side(side_ref, f, level, levels),
                from_side(side_rim_ref, f, level, levels),
                from_side(next_side_ref, f, level, levels),
                tiles,
                keep,
            )
            state[tile_at(f * levels + level), :] = q
            out.append(q)
        xs[level] = jnp.concatenate(out, 0).astype(jnp.bfloat16)
        return carry

    each_level(levels, transport, 0, 4)

    diffuse = diffuse_factor * tau_scale
    pairs = levels // 2
    depths[0][0] = jnp.zeros((groups, ROWS, COLS), jnp.float32)
    depths[1][0] = jnp.zeros((groups, ROWS, COLS), jnp.float32)
    ones = jnp.ones((w3.shape[1] - hid, 2 * COLS), jnp.bfloat16)

    def silu(half):
        return (half + half * jnp.tanh(half)).astype(jnp.bfloat16)

    def layer_one(pair, out):
        x = jnp.concatenate(
            [jnp.concatenate([gases[2 * pair + k], xs[2 * pair + k]], 0) for k in range(2)], 1
        )
        wide = jnp.concatenate([b1[...]] * 2, 1)
        part = ROWS // 2
        for at in range(0, ROWS, part):
            mine = w1[at * hid : (at + part) * hid, :]
            y = jnp.dot(mine, x, preferred_element_type=jnp.float32)
            for k in range(part):
                out[(at + k) * hid : (at + k + 1) * hid, :] = silu(
                    y[k * hid : (k + 1) * hid] + wide
                )

    def layer_two(pair, source, at=lambda row, pair: row * pairs + pair):
        wide = jnp.concatenate([b2[...]] * 2, 1)
        for row in range(ROWS):
            y = source[row * hid : (row + 1) * hid, :]
            y = silu(jnp.dot(w2[...], y, preferred_element_type=jnp.float32) + wide)
            hidden[at(row, pair)] = jnp.concatenate([y, ones], 0)

    def layers(step, carry):
        layer_one(2 * step, hid_a)

        layer_two(
            2 * step - 1,
            hid_b,
            lambda row, pair: jnp.where(step == 0, ROWS * pairs, row * pairs + pair),
        )

        layer_one(2 * step + 1, hid_b)
        layer_two(2 * step, hid_a)
        return carry

    lax.fori_loop(0, pairs // 2, layers, 0)
    layer_two(pairs - 1, hid_b)

    def third(at, buf):
        buf[...] = jnp.dot(w3[...], hidden[at], preferred_element_type=jnp.float32).reshape(
            groups, ROWS, 2 * COLS
        )

    def optical(pair, depth, buf):
        t = buf[...] * log2e
        soft = jnp.maximum(t, jnp.log2(1.0 + jnp.exp2(jnp.minimum(t, 126.0))))
        d = depth[2 * pair] + soft[:, :, :COLS]
        depth[2 * pair + 1] = d
        depth[2 * pair + 2] = d + soft[:, :, COLS:]

    def light(row, level, depth):
        d = depth[level]
        direct = jnp.exp2(lsolar[...] - d * kappa[row][None])
        upward = jnp.exp2(weight[...] + d * diffuse)
        sums[row, level] = jnp.sum(direct - upward, 0)

    def close(row, depth):
        total = depth[levels]
        weight[...] = (
            lsolar[...] + lground[row][None] - total * (kappa[row] + diffuse)[None]
        )
        light(row, levels, depth)

    def both(row, depth, before):
        close(row - 1, before)

        def step(trip, carry):
            for k, buf in enumerate(bufs):
                pair = 2 * trip + k
                optical(pair, depth, buf)
                light(row - 1, 2 * pair, before)
                light(row - 1, 2 * pair + 1, before)
                third(row * pairs + pair + 2, buf)
            return carry

        lax.fori_loop(0, pairs // 2, step, 0)

    def only_optical(trip, carry):
        for k, buf in enumerate(bufs):
            optical(2 * trip + k, depths[0], buf)
            third(2 * trip + k + 2, buf)
        return carry

    bufs = (logits_a, logits_b)
    third(0, logits_a)
    third(1, logits_b)
    lax.fori_loop(0, pairs // 2, only_optical, 0)

    def two_rows(step, carry):
        both(2 * step + 1, depths[1], depths[0])
        both(2 * step + 2, depths[0], depths[1])
        return carry

    lax.fori_loop(0, ROWS // 2 - 1, two_rows, 0)
    both(ROWS - 1, depths[1], depths[0])
    close(ROWS - 1, depths[1])

    def only_light(pair, carry):
        light(ROWS - 1, 2 * pair, depths[1])
        light(ROWS - 1, 2 * pair + 1, depths[1])
        return carry

    lax.fori_loop(0, pairs, only_light, 0)

    for row in range(ROWS):
        change = sums[row, 0:levels] - sums[row, 1 : levels + 1]
        heating[:, row, :] = jnp.sum(change, 1) * scaled[row : row + 1, :]

    def add(level, carry):
        tile = tile_at(level)
        state[tile, :] = state[tile, :] + heating[level]
        return carry

    each_level(levels, add, 0, 8)
    pack_rows((state,), lat_even, next_rows_one, next_rows_two)
    pack_fields(
        [lambda level, f=f: state[tile_at(f * levels + level), :] for f in range(ntr)],
        levels,
        lon_even,
        next_one,
        next_two,
    )


def last_kernel(
    tracers,
    face,
    side_face,
    own_one,
    own_two,
    cols_one,
    cols_two,
    rows_one,
    rows_two,
    flags,
    out,
    rim_ref,
    corner_ref,
    side_ref,
    next_side_ref,
    side_rim_ref,
):
    ntr, levels = out.shape[0], out.shape[1]
    packed = packed_tiles(ntr, levels)
    lon_even, lat_even = flags[LON_EVEN, 0:1], flags[LAT_EVEN, 0:1]
    unpack_rows(lat_even, rows_one, rows_two, rim_ref, corner_ref, ntr * levels, packed)
    keep = kept_rows(flags)
    of_sides = [side_face[k] for k in range(4)]
    for tile in range(packed):
        sides = side_tiles(
            lon_even, own_one, own_two, cols_one, cols_two, corner_ref, tile, packed
        )
        side_ref[tile] = sides[0]
        side_rim_ref[tile] = sides[3]
        next_side_ref[tile] = side_step(sides, of_sides)

    def transport(level, carry):
        tiles = [face[level, k] for k in range(6)]
        for f in range(ntr):
            out[f, level] = two_steps(
                tracers[tile_at(f * levels + level), :],
                rim_ref[tile_at(f * levels + level), :],
                from_side(side_ref, f, level, levels),
                from_side(side_rim_ref, f, level, levels),
                from_side(next_side_ref, f, level, levels),
                tiles,
                keep,
            )
        return carry

    each_level(levels, transport, 0, 4)


def prepare_kernel(
    index,
    slot,
    ground,
    table,
    solar,
    w_first,
    b_first,
    w_second,
    b_second,
    w_third,
    b_third,
    w1,
    b1,
    w2,
    b2,
    w3,
    lsolar,
    kappa,
    lground,
    scaled,
    square,
    wide,
):
    feat, hid = w_first.shape
    bands = solar.shape[1]

    def column(ref, factor):
        square[:, 0 : ref.shape[1]] = jnp.broadcast_to(ref[...], (COLS, ref.shape[1])) * factor
        return jnp.transpose(square[...])[0 : ref.shape[1]]

    square[...] = jnp.zeros(square.shape, jnp.float32)
    b1[...] = column(b_first, 0.5)
    b2[...] = column(b_second, 0.5)

    square[...] = jnp.zeros(square.shape, jnp.float32)
    square[0:hid, 0:hid] = w_second[...].astype(jnp.float32) * 0.5
    w2[...] = jnp.transpose(square[...])[0:hid, 0:hid].astype(jnp.bfloat16)

    square[...] = jnp.zeros(square.shape, jnp.float32)
    square[0:feat, 0:hid] = w_first[...].astype(jnp.float32) * 0.5
    by_unit = jnp.transpose(square[...])[0:hid].astype(jnp.bfloat16)
    source = lax.broadcasted_iota(jnp.int32, (COLS, COLS), 0)
    lane = lax.broadcasted_iota(jnp.int32, (COLS, COLS), 1)
    spread = jnp.where(lane // ROWS == source, 1.0, 0.0).astype(jnp.bfloat16)
    by_lane = jnp.dot(by_unit, spread, preferred_element_type=jnp.float32)
    of_row = lax.broadcasted_iota(jnp.int32, (hid, COLS), 1) % ROWS
    for row in range(ROWS):
        w1[row * hid : (row + 1) * hid, :] = jnp.where(of_row == row, by_lane, 0.0).astype(
            jnp.bfloat16
        )

    wide[...] = jnp.zeros(wide.shape, jnp.float32)
    wide[0:hid, 0:bands] = w_third[...].astype(jnp.float32)
    rest = b_third[...]
    for k in range(3):
        part = rest.astype(jnp.bfloat16).astype(jnp.float32)
        wide[hid + k : hid + k + 1, 0:bands] = part
        rest = rest - part
    w3[...] = jnp.transpose(wide[...])[0:bands, 0 : w3.shape[1]].astype(jnp.bfloat16)

    wide[:, 0:bands] = jnp.broadcast_to(jnp.log2(solar[...]), (COLS, bands))
    lsolar[...] = jnp.transpose(wide[...])[0:bands].reshape(lsolar.shape)

    ids = index[...]
    cosine = jnp.zeros((ROWS, COLS), jnp.float32)
    for entry in range(1, table.shape[0]):
        cosine = jnp.where(ids == entry, table[entry], cosine)
    slant = tau_scale / jnp.maximum(cosine, mu_floor)
    lg = jnp.log2(ground[...].astype(jnp.float32))
    for row in range(ROWS):
        kappa[row] = jnp.broadcast_to(slant[row : row + 1], (ROWS, COLS))
        lground[row] = jnp.broadcast_to(lg[row : row + 1], (ROWS, COLS))
        lit = jnp.where(slot[0, row] >= 0, heat_scale, 0.0)
        scaled[row : row + 1, :] = lit * cosine[row : row + 1]


vmem = pl.BlockSpec(memory_space=pltpu.VMEM)
smem = pl.BlockSpec(memory_space=pltpu.SMEM)
f32 = jnp.float32


def tiles_like(*shape):
    return jax.ShapeDtypeStruct(shape, f32)


def held(*shape, dtype=f32):
    return pltpu.VMEM(shape, dtype)


def near(*arrays):
    return [pltpu.with_memory_space_constraint(x, pltpu.VMEM) for x in arrays]


def swap_pairs(one, two, axis, ring):
    count = lax.axis_size(axis)
    near = [(i, i ^ 1) for i in range(count)]
    far = [(i, (i - 1 if i % 2 == 0 else i + 1) % count) for i in range(count)]
    if not ring:
        far = [(i, j) for i, j in far if abs(i - j) == 1]
    return lax.ppermute(one, axis, near), lax.ppermute(two, axis, far)


def add_corners(one, two, flags, cols):
    return pl.pallas_call(
        corner_kernel,
        in_specs=[vmem] * 5,
        out_specs=[vmem] * 2,
        out_shape=[held(*one.shape)] * 2,
        input_output_aliases={0: 0, 1: 1},
        name="add_corners",
    )(*near(one, two, flags, *cols))


def body(
    tracers,
    winds,
    gases,
    sun_index,
    block_slot,
    albedo,
    sun_table,
    solar,
    w_first,
    b_first,
    w_second,
    b_second,
    w_third,
    b_third,
):
    ntr, levels, clat, width = tracers.shape
    fields = ntr + winds.shape[0]
    gas = gases.shape[0]
    hid = w_first.shape[1]
    bands = solar.shape[0]
    if lax.axis_size("lat") % 2 or lax.axis_size("lon") % 2:
        raise ValueError("unsupported mesh")
    if (clat, width) != (ROWS, COLS) or w_first.shape[0] * ROWS != COLS or levels % 8 or 2 * levels != SLOTS or ntr % 2 or SLOTS % levels or bands % ROWS:
        raise ValueError("unsupported sizes")

    flat = (tracers.reshape(-1, COLS), winds.reshape(-1, COLS))
    columns = held(packed_tiles(fields, levels), ROWS, COLS)
    lat, lats = lax.axis_index("lat"), lax.axis_size("lat")
    flags = [lat < lats - 1, lat > 0, lat % 2 == 0, lax.axis_index("lon") % 2 == 0]
    flags = jnp.stack(flags).astype(f32)[:, None, None]
    flags = jnp.broadcast_to(flags, (4, ROWS, COLS))
    one, two, rows_one, rows_two = pl.pallas_call(
        functools.partial(pack_kernel, levels),
        in_specs=[vmem] * 3,
        out_specs=[vmem] * 4,
        out_shape=[columns] * 2 + [held(row_payload(fields, levels), COLS)] * 2,
        name="pack",
    )(*near(flags), *flat)
    own = (one, two)
    cols = swap_pairs(one, two, "lon", True)

    rows = add_corners(rows_one, rows_two, flags, cols)
    rows, gases, sun_index = lax.optimization_barrier((rows, gases, sun_index))

    groups = bands // ROWS
    bf16 = jnp.bfloat16
    prepared = pl.pallas_call(
        prepare_kernel,
        in_specs=[vmem, smem, vmem, smem] + [vmem] * 7,
        out_specs=[vmem] * 9,
        out_shape=[
            held(ROWS * hid, w_first.shape[0] * ROWS, dtype=bf16),
            held(hid, COLS),
            held(hid, hid, dtype=bf16),
            held(hid, COLS),
            held(bands, hid + 16, dtype=bf16),
            held(groups, ROWS, COLS),
            held(ROWS, ROWS, COLS),
            held(ROWS, ROWS, COLS),
            held(ROWS, COLS),
        ],
        scratch_shapes=[
            pltpu.VMEM((COLS, COLS), f32),
            pltpu.VMEM((COLS, pl.cdiv(bands, COLS) * COLS), f32),
        ],
        name="prepare",
    )(
        sun_index,
        block_slot.reshape(1, -1),
        albedo,
        sun_table,
        solar.reshape(1, -1),
        w_first,
        b_first.reshape(1, -1),
        w_second,
        b_second.reshape(1, -1),
        w_third,
        b_third.reshape(1, -1),
    )
    gas_rows = gases.transpose(1, 0, 2, 3).reshape(levels, gas * ROWS, COLS)
    rows = swap_pairs(*rows, "lat", False)

    packed = packed_tiles(fields, levels)
    state, heating, one, two, rows_one, rows_two, face, side_face = pl.pallas_call(
        first_kernel,
        in_specs=[vmem] * 19,
        out_specs=[vmem] * 8,
        out_shape=[held(ntr * levels * ROWS, COLS), tiles_like(levels, ROWS, COLS)]
        + [held(packed_tiles(ntr, levels), ROWS, COLS)] * 2
        + [held(row_payload(ntr, levels), COLS)] * 2
        + [held(levels, 6, ROWS, COLS), held(4, ROWS, COLS)],
        scratch_shapes=[
            pltpu.VMEM((fields * levels * ROWS, COLS), f32),
            pltpu.VMEM((2 * packed, ROWS, COLS), f32),
            pltpu.VMEM((packed, ROWS, COLS), f32),
            pltpu.VMEM((packed, ROWS, COLS), f32),
            pltpu.VMEM((packed, ROWS, COLS), f32),
            pltpu.VMEM((levels, ntr * ROWS, COLS), bf16),
            pltpu.VMEM((ROWS * hid, 2 * COLS), bf16),
            pltpu.VMEM((ROWS * hid, 2 * COLS), bf16),
            pltpu.VMEM((ROWS * levels // 2 + 2, hid + 16, 2 * COLS), bf16),
            pltpu.VMEM((groups, ROWS, 2 * COLS), f32),
            pltpu.VMEM((groups, ROWS, 2 * COLS), f32),
            pltpu.VMEM((levels + 1, groups, ROWS, COLS), f32),
            pltpu.VMEM((levels + 1, groups, ROWS, COLS), f32),
            pltpu.VMEM((groups, ROWS, COLS), f32),
            pltpu.VMEM((ROWS, levels + 1, ROWS, COLS), f32),
        ],
        compiler_params=pltpu.CompilerParams(vmem_limit_bytes=28 << 20),
        name="transport_radiation",
    )(*near(tracers, winds, *own, *cols, *rows, flags, gas_rows, *prepared))

    own = (one, two)
    cols = swap_pairs(one, two, "lon", True)
    rows = swap_pairs(*add_corners(rows_one, rows_two, flags, cols), "lat", False)
    final = pl.pallas_call(
        last_kernel,
        in_specs=[vmem] * 10,
        out_specs=vmem,
        out_shape=tiles_like(ntr, levels, ROWS, COLS),
        scratch_shapes=[
            pltpu.VMEM((ntr * levels * ROWS, COLS), f32),
            pltpu.VMEM((2 * packed_tiles(ntr, levels), ROWS, COLS), f32),
        ]
        + [pltpu.VMEM((packed_tiles(ntr, levels), ROWS, COLS), f32)] * 3,
        compiler_params=pltpu.CompilerParams(vmem_limit_bytes=8 << 20),
        name="last_transport",
    )(*near(state, face, side_face, *own, *cols, *rows, flags))
    return final, heating


def solution(mesh):
    grid = P(None, None, "lat", "lon")
    in_specs = (grid, grid, grid) + (P("lat", "lon"),) * 3 + (P(),) * 8
    out_specs = (grid, P(None, "lat", "lon"))
    return jax.shard_map(body, mesh=mesh, in_specs=in_specs, out_specs=out_specs, check_vma=False)
```
